128 devices in a mesh: dp: 32 (over z, y, x_hi), blk: 4 (over x_lo, core).
Axes of the slice: x: 4 (x_hi: 2, x_lo: 2; x = x_hi * 2 + x_lo), y: 4, z: 4, core: 2. Of those that a mesh axis runs over, the one named last changes fastest.
Arguments:
- tokens: bfloat16 [16384, 4096], P(('dp', 'blk')), may hold values from -6 to 6
- gate_projection_weight: bfloat16 [4096, 7168], P(None, 'blk'), may hold values from -0.09375 to 0.09375
- up_projection_weight: bfloat16 [4096, 7168], P('dp', 'blk'), may hold values from -0.09375 to 0.09375
- down_projection_weight: bfloat16 [7168, 4096], P('blk', 'dp'), may hold values from -0.0625 to 0.0625
- router_projection_weight: bfloat16 [4096, 8], replicated, may hold values from -0.09375 to 0.09375
- adapter_down_factors: bfloat16 [4096, 128], replicated, may hold values from -0.09375 to 0.09375
- adapter_up_factors: bfloat16 [128, 4096], replicated, may hold values from -1.5 to 1.5
- routes: int32 [16384, 2], P(('dp', 'blk')), may hold values from 0 to 7, all different within a row
- padding_token_mask: int32 [16384], P(('dp', 'blk')), may hold values 0 or 1
- cotangent: bfloat16 [16384, 4096], P(('dp', 'blk')), may hold values from -6 to 6
Outputs:
- layer_out: bfloat16 [16384, 4096], P(('dp', 'blk'))
- grad_down: float32 [4096, 128], replicated
- grad_up: float32 [128, 4096], replicated
The draws below stay inside these ranges and needn't reach their ends.
Inputs may be any that keep to these rules, and one draw needn't show every extreme that they name: `routes`: the two experts of a token differ.
All inputs are finite; a program needn't handle non-finite values. No bound on the sum of `padding_token_mask` on one device may be relied on, other than what follows from the above.
Results may differ from the reference program's by a relative error of at most 0.0075.
Values may be sent and summed in bfloat16 or wider, within the bound.
A program may use at most 192 MiB of HBM per device.

```python
import jax
import jax.numpy as jnp
from jax import lax

MODEL_WIDTH = 4096
FF = 7168
EXPERTS = 8
EXPERT_RANK = 16
TOKENS = 16384
LOW_RANK_COLUMNS = 128
N_BLK = 4


def place_ends(result, own_key, least, top_value):
    spot = [jax.random.randint(jax.random.fold_in(own_key, axis), (), 0, length) for axis, length in enumerate(result.shape)]
    longest = result.shape.index(max(result.shape))
    beside = spot[:longest] + [(spot[longest] + 1) % result.shape[longest]] + spot[longest + 1:]
    return result.at[tuple(spot)].set(least).at[tuple(beside)].set(top_value)


def shard_levels(own_key, shape, shards, low, top_value):
    loudness, own = 1.0, jax.random.fold_in(own_key, 6)
    for dim, blocks in shards:
        draws = jnp.exp(jax.random.uniform(jax.random.fold_in(own, dim), (blocks,), jnp.float32, low / len(shards), top_value / len(shards)))
        loudness = loudness * jnp.repeat(draws, shape[dim] // blocks).reshape([-1 if axis == dim else 1 for axis in range(len(shape))])
    return loudness


def choose_distinct(rng, rows, count, top, lift):
    order = jax.random.permutation(jax.random.fold_in(rng, 1), count)
    boost = order
    for power in range(3):
        boost = boost * boost // count
    boost = boost * lift // count
    chance = jax.random.randint(jax.random.fold_in(rng, 2), (rows, count), 0, 4096) + boost
    holders = jax.random.permutation(jax.random.fold_in(rng, 3), rows)[jnp.arange(count) % rows]
    chance = jnp.where(jnp.arange(rows)[:, None] == holders[None, :], 1 << 14, chance)
    merit = chance * count + jnp.arange(count)
    return lax.top_k(merit.astype(jnp.int32), top)[1].astype(jnp.int32)


def centred(stream_key, extent, scale, most, shards=(), kind=jnp.bfloat16):
    level = shard_levels(stream_key, extent, shards, -0.22, 0.18) if shards else 1.0
    array = jax.random.normal(stream_key, extent, jnp.float32) * scale * level
    return jnp.minimum(jnp.maximum(array, -most), most).astype(kind)


def setup_inputs(seed: int = 0) -> dict:
    splits = jax.random.split(jax.random.key(seed), 11)
    return {
        "tokens": centred(splits[0], (TOKENS, MODEL_WIDTH), 1.0, 6.0, ((0, 128),)),
        "gate_projection_weight": centred(splits[1], (MODEL_WIDTH, FF), MODEL_WIDTH ** -0.5, 0.09375, ((1, 4),)),
        "up_projection_weight": centred(splits[2], (MODEL_WIDTH, FF), MODEL_WIDTH ** -0.5, 0.09375, ((0, 32), (1, 4))),
        "down_projection_weight": centred(splits[3], (FF, MODEL_WIDTH), FF ** -0.5, 0.0625, ((0, 4), (1, 32))),
        "router_projection_weight": centred(splits[4], (MODEL_WIDTH, EXPERTS), MODEL_WIDTH ** -0.5, 0.09375),
        "adapter_down_factors": centred(splits[5], (MODEL_WIDTH, LOW_RANK_COLUMNS), MODEL_WIDTH ** -0.5, 0.09375),
        "adapter_up_factors": centred(splits[6], (LOW_RANK_COLUMNS, MODEL_WIDTH), EXPERT_RANK ** -0.5, 1.5),
        "routes": choose_distinct(splits[7], TOKENS, EXPERTS, 2, 2048),
        "padding_token_mask": place_ends((jax.random.randint(splits[8], (TOKENS,), 0, 8) < 7).astype(jnp.int32), jax.random.fold_in(splits[8], 1), 0, 1),
        "cotangent": centred(splits[9], (TOKENS, MODEL_WIDTH), 1.0, 6.0, ((0, 128),)),
    }


def reference(tokens, gate_projection_weight, up_projection_weight, down_projection_weight, router_projection_weight, adapter_down_factors, adapter_up_factors, routes, padding_token_mask, cotangent):
    width = FF // N_BLK
    base = jnp.zeros((tokens.shape[0], tokens.shape[1]), jnp.float32)
    for group in range(N_BLK):
        lower = group * width
        gate_act = jnp.dot(tokens, gate_projection_weight[:, lower:lower + width], preferred_element_type=jnp.float32)
        up_act = jnp.dot(tokens, up_projection_weight[:, lower:lower + width], preferred_element_type=jnp.float32)
        hidden = (jax.nn.silu(gate_act) * up_act).astype(jnp.bfloat16)
        part = jnp.dot(hidden, down_projection_weight[lower:lower + width, :], preferred_element_type=jnp.float32)
        part = lax.optimization_barrier(part.astype(jnp.bfloat16))
        base = base + part.astype(jnp.float32)
    logits = jnp.dot(tokens, router_projection_weight, preferred_element_type=jnp.float32)
    experts_iota = jnp.arange(EXPERTS, dtype=jnp.int32)[None, :]
    first_hot = (routes[:, 0:1] == experts_iota).astype(jnp.float32)
    second_hot = (routes[:, 1:2] == experts_iota).astype(jnp.float32)
    first_logit = jnp.sum(logits * first_hot, axis=1, keepdims=True)
    second_logit = jnp.sum(logits * second_hot, axis=1, keepdims=True)
    weight_first = jax.nn.sigmoid(first_logit - second_logit)
    coeff = weight_first * first_hot + (1.0 - weight_first) * second_hot
    coeff_wide = jnp.repeat(coeff, EXPERT_RANK, axis=1)
    low_rank_state = jnp.dot(tokens, adapter_down_factors, preferred_element_type=jnp.float32)
    scaled_output = (low_rank_state * coeff_wide).astype(jnp.bfloat16)
    adapter_delta = jnp.dot(scaled_output, adapter_up_factors, preferred_element_type=jnp.float32)
    layer_out = (base + adapter_delta).astype(jnp.bfloat16)
    masked_tokens = cotangent * padding_token_mask[:, None].astype(jnp.bfloat16)
    low_rank_gradient = lax.dot_general(masked_tokens, adapter_up_factors, (((1,), (1,)), ((), ())), preferred_element_type=jnp.float32)
    dlow = (low_rank_gradient * coeff_wide).astype(jnp.bfloat16)
    live = jnp.sum(padding_token_mask.astype(jnp.float32))
    inverse = 1.0 / jnp.maximum(live, 1.0)
    grad_up = lax.dot_general(scaled_output, masked_tokens, (((0,), (0,)), ((), ())), preferred_element_type=jnp.float32) * inverse
    grad_down = lax.dot_general(tokens, dlow, (((0,), (0,)), ((), ())), preferred_element_type=jnp.float32) * inverse
    return layer_out, grad_down, grad_up
```

```python
import jax
import jax.numpy as jnp
from jax import lax
from jax.experimental import pallas as pl
from jax.experimental.pallas import tpu as pltpu
from jax.sharding import PartitionSpec as P

MESH = pl.DeviceIdType.MESH
BF, F32 = jnp.bfloat16, jnp.float32

REL = (0, 1, 3, 2)
LINK_RATE, PAIR_RATE = 46.6e3, 300e3
HOP, PAIR_HOP = 1.8, 1.0


class Copy:
    def __init__(self, name, link, size, source, landing, here, hops=1):
        self.name, self.link, self.size, self.hops = name, link, size, hops
        self.target = "xx" if hops == 2 else link
        self.source, self.landing, self.here = source, landing, here
        self.after = set()


class Task:
    def __init__(self, name, cost, run, after, rank):
        self.name, self.cost, self.run, self.after, self.rank = name, cost, run, set(after), rank


def arrange(copies, tasks, begun):
    order, done, now = [], set(begun), 0.0
    free, arriving = {}, []
    to_send, to_run = list(copies), list(tasks)

    def send_ready():
        for copy in list(to_send):
            if copy.after <= done:
                to_send.remove(copy)
                order.append(("send", copy))
                rate, hop = (PAIR_RATE, PAIR_HOP) if copy.link == "pair" else (LINK_RATE, HOP)
                start = max(now, free.get(copy.link, 0.0))
                end = start + copy.size * copy.hops / rate
                free[copy.link] = end
                arriving.append((end + hop * copy.hops, copy))

    send_ready()
    while arriving or to_run:
        arriving.sort(key=lambda pair: pair[0])
        ready = [task for task in to_run if task.after <= done]
        if arriving and arriving[0][0] <= now:
            copy = arriving.pop(0)[1]
            order.append(("recv", copy))
            done.add(copy.name)
            send_ready()
        elif ready:
            task = min(ready, key=lambda task: task.rank)
            to_run.remove(task)
            order.append(("task", task))
            now += task.cost
            done.add(task.name)
            send_ready()
        else:
            now = arriving[0][0]
    assert not to_send
    return order, now


def kernel(tokens, gate, up, down, base, tok, gw, ub, db, gact, uact, hid, psib, rsib, summed,
           rl, rr, fl, fr, load_sem, send_sem, recv_sem):
    dp, blk = lax.axis_index("dp"), lax.axis_index("blk")
    z, y, xh = dp // 8, (dp // 2) % 4, dp % 2
    xl, core = blk // 2, blk % 2
    x = xh * 2 + xl

    def device(dz=0, dy=0, dx=0, dc=0):
        at_z, at_y, at_x = (z + dz) % 4, (y + dy) % 4, (x + dx) % 4
        return ((at_z * 4 + at_y) * 2 + at_x // 2, (at_x % 2) * 2 + (core + dc) % 2)

    targets = {
        "z+": device(dz=1), "z-": device(dz=3), "y+": device(dy=1), "y-": device(dy=3),
        "x+": device(dx=1), "x-": device(dx=3), "xx": device(dx=2), "pair": device(dc=1),
    }

    def plane(dz, dy):
        return ((z + dz) % 4) * 4 + (y + dy) % 4

    copies = []

    def add(name, link, size, source, landing, here, after=(), hops=1):
        copy = Copy(name, link, size, source, landing, here, hops)
        copy.after = set(after)
        copies.append(copy)
        return copy

    piece = 128 * 896 * 2

    def weight(kind, dz, dy, own, half=None):
        ref, rows = (ub, 128) if kind == "u" else (db, 896)
        ref = ref.at[plane(dz, dy), xh if own else 1 - xh]
        if half is None:
            return ref
        return ref.at[pl.ds(half * (rows // 2), rows // 2)]

    def spread(kind, own, first, origin):
        tag = kind + ("o" if own else "p")
        second = "z" if first == "y" else "y"

        def at(f, s, half=None):
            dz, dy = (f, s) if first == "z" else (s, f)
            return weight(kind, dz, dy, own, half)

        def move(name, link, f, s, f_new, s_new, after, half=None):
            size = piece if half is None else piece // 2
            add(tag + name, link, size, at(f, s, half), at(f, s, half), at(f_new, s_new, half), after)

        move("F+", first + "+", 0, 0, 3, 0, [origin])
        move("F-", first + "-", 0, 0, 1, 0, [origin])
        move("S+0", second + "+", 0, 0, 0, 3, [origin])
        move("S-0", second + "-", 0, 0, 0, 1, [origin])
        move("G+", first + "+", 3, 0, 2, 0, [tag + "F+"], 0)
        move("G-", first + "-", 1, 0, 2, 0, [tag + "F-"], 1)
        came = {0: [origin], 3: [tag + "F+"], 1: [tag + "F-"], 2: [tag + "G+", tag + "G-"]}
        for f in REL[1:]:
            move("S+%d" % f, second + "+", f, 0, f, 3, came[f])
            move("S-%d" % f, second + "-", f, 0, f, 1, came[f])
        for f in (0, 1):
            move("T+%d" % f, second + "+", f, 3, f, 2, [tag + "S+%d" % f])
        for f in (3, 2):
            move("T-%d" % f, second + "-", f, 1, f, 2, [tag + "S-%d" % f])

        def have(f, s):
            if s == 0:
                return came[f]
            if s == 3:
                return [tag + "S+%d" % f]
            if s == 1:
                return [tag + "S-%d" % f]
            return [tag + ("T+%d" if f in (0, 1) else "T-%d") % f]

        return (lambda dz, dy: have(dz, dy)) if first == "z" else (lambda dz, dy: have(dy, dz))

    other = 1 - xh
    add("AU", "x+", piece, up.at[:, pl.ds(pl.multiple_of(other * 896, 128), 896)], ub.at[plane(0, 0), xh], ub.at[plane(0, 0), other], hops=2)
    mib = 128 * 4096 * 2
    add("K+", "x+", mib, tok.at[0, 0], tok.at[3, 0], tok.at[3, 0], ["L"])
    add("K-", "x-", mib, tok.at[0, 0], tok.at[1, 0], tok.at[1, 0], ["L"])
    add("KS0", "pair", mib, tok.at[0, 0], tok.at[0, 1], tok.at[0, 1], ["L"])
    add("AD", "x+", piece, down.at[pl.ds(pl.multiple_of(other * 896, 128), 896), :], db.at[plane(0, 0), xh], db.at[plane(0, 0), other], hops=2)
    have_uo = spread("u", True, "y", "L")
    have_up = spread("u", False, "z", "AU")
    have_do = spread("d", True, "z", "L")
    have_dp = spread("d", False, "y", "AD")
    low, high = pl.ds(0, 64), pl.ds(64, 64)
    add("KF+", "x+", mib // 2, tok.at[3, 0, low], tok.at[2, 0, low], tok.at[2, 0, low], ["K+"])
    add("KF-", "x-", mib // 2, tok.at[1, 0, high], tok.at[2, 0, high], tok.at[2, 0, high], ["K-"])
    add("KS3", "pair", mib, tok.at[3, 0], tok.at[3, 1], tok.at[3, 1], ["K+"])
    add("KS1", "pair", mib, tok.at[1, 0], tok.at[1, 1], tok.at[1, 1], ["K-"])
    add("KS2", "pair", mib, tok.at[2, 0], tok.at[2, 1], tok.at[2, 1], ["KF+", "KF-"])
    came_tok = {0: ["L", "KS0"], 3: ["K+", "KS3"], 1: ["K-", "KS1"], 2: ["KF+", "KF-", "KS2"]}

    tasks = []

    def project(r, weights, act, start):
        def step(i, carry):
            k = pl.multiple_of(i * 512, 512)
            left = tok[r, :, :, pl.ds(k, 512)].reshape(256, 512)
            part = jnp.dot(left, weights(i), preferred_element_type=F32)
            act[...] += part
            return carry

        act[...] = jnp.zeros_like(act)
        lax.fori_loop(0, 8, step, 0)

    def run_gate(r):
        def run():
            project(r, lambda i: gw[pl.ds(pl.multiple_of(i * 512, 512), 512), :], uact, 0)
            v = uact[...]
            gact[r] = v / (1.0 + jnp.exp(-v))
        return run

    def run_up(r):
        def run():
            project(r, lambda i: ub[pl.ds(i * 2, 2)].reshape(512, 896), uact, 0)
            hid[r] = (gact[r] * uact[...]).astype(BF)
        return run

    every_up = [n for dz in range(4) for dy in range(4) for n in have_uo(dz, dy) + have_up(dz, dy)]
    for rank, r in enumerate(REL):
        tasks.append(Task("G%d" % r, 2.6, run_gate(r), came_tok[r] + ["LG"], 10 + rank))
        tasks.append(Task("U%d" % r, 2.8, run_up(r), every_up + ["G%d" % r], 1 + rank))

    blocks = sorted(((dz, dy) for dz in range(4) for dy in range(4)), key=lambda p: (min(p[0], 4 - p[0]) + min(p[1], 4 - p[1]), p))
    size = 128 * 256 * 2

    def run_down(b, dz, dy):
        def run():
            j = plane(dz, dy)
            right = jnp.concatenate([db[j, 0], db[j, 1]], axis=1)

            def step(i, carry):
                left = hid[pl.ds(i * 2, 2)].reshape(512, 896)
                part = jnp.dot(left, right, preferred_element_type=F32).astype(BF).reshape(2, 2, 128, 256)
                summed[b, pl.ds(i * 2, 2)] = part[:, 0]
                psib[b, pl.ds(i * 2, 2)] = part[:, 1]
                return carry

            lax.fori_loop(0, 2, step, 0)
        return run

    def run_add(b):
        def run():
            summed[b] = (summed[b].astype(F32) + rsib[b].astype(F32)).astype(BF)
        return run

    def run_merge(b):
        def run():
            if b % 2 == 0:
                summed[b, 1] = (summed[b, 1].astype(F32) + rl[b // 2].astype(F32)).astype(BF)
            else:
                summed[b, 3] = (summed[b, 3].astype(F32) + rr[b // 2].astype(F32)).astype(BF)
        return run

    def run_final(b, dz, dy):
        def run():
            total = summed[b, 0].astype(F32) + fl[b].astype(F32) + fr[b].astype(F32)
            base[:, pl.ds(pl.multiple_of(plane(dz, dy) * 256, 256), 256)] = total
        return run

    hidden = ["U%d" % r for r in range(4)]
    for b, (dz, dy) in enumerate(blocks):
        n, half = str(b), b // 2
        tasks.append(Task("D" + n, 0.9, run_down(b, dz, dy), hidden + have_do(dz, dy) + have_dp(dz, dy), 300 + b))
        add("Q" + n, "pair", 4 * size, psib.at[b], rsib.at[b], rsib.at[b], ["D" + n])
        tasks.append(Task("A" + n, 0.15, run_add(b), ["D" + n, "Q" + n], 200 + b))
        if b % 2 == 0:
            add("Z" + n, "x+", size, summed.at[b, 2], rl.at[half], rl.at[half], ["A" + n])
            add("N" + n, "x-", size, summed.at[b, 3], fr.at[b], fr.at[b], ["A" + n])
            add("M" + n, "x+", size, summed.at[b, 1], fl.at[b], fl.at[b], ["C" + n])
        else:
            add("Z" + n, "x-", size, summed.at[b, 2], rr.at[half], rr.at[half], ["A" + n])
            add("N" + n, "x+", size, summed.at[b, 1], fl.at[b], fl.at[b], ["A" + n])
            add("M" + n, "x-", size, summed.at[b, 3], fr.at[b], fr.at[b], ["C" + n])
        tasks.append(Task("C" + n, 0.05, run_merge(b), ["A" + n, "Z" + n], 100 + b))
        tasks.append(Task("E" + n, 0.1, run_final(b, dz, dy), ["A" + n, "M" + n, "N" + n], 400 + b))

    order, _ = arrange(copies, tasks, ["L", "LG"])
    place = {copy.name: i for i, copy in enumerate(copies)}

    def descriptor(copy, landing):
        i = place[copy.name]
        return pltpu.make_async_remote_copy(
            src_ref=copy.source, dst_ref=landing, send_sem=send_sem.at[i], recv_sem=recv_sem.at[i],
            device_id=targets[copy.target], device_id_type=MESH)

    loads = [
        pltpu.make_async_copy(tokens, tok.at[0, 0], load_sem.at[0]),
        pltpu.make_async_copy(up.at[:, pl.ds(pl.multiple_of(xh * 896, 128), 896)], ub.at[plane(0, 0), xh], load_sem.at[1]),
        pltpu.make_async_copy(down.at[pl.ds(pl.multiple_of(xh * 896, 128), 896), :], db.at[plane(0, 0), xh], load_sem.at[2]),
    ]
    load_gate = pltpu.make_async_copy(gate.at[:, pl.ds(pl.multiple_of(xh * 896, 128), 896)], gw, load_sem.at[3])
    for load in loads:
        load.start()
    load_gate.start()
    barrier = pltpu.get_barrier_semaphore()
    for target in targets.values():
        pl.semaphore_signal(barrier, inc=1, device_id=target, device_id_type=MESH)
    pl.semaphore_wait(barrier, len(targets))
    for load in loads:
        load.wait()
    gate_waited = False
    for what, item in order:
        if what == "send":
            descriptor(item, item.landing).start()
        elif what == "recv":
            descriptor(item, item.here).wait_recv()
        else:
            if item.name[0] == "G" and not gate_waited:
                load_gate.wait()
                gate_waited = True
            item.run()
    for copy in copies:
        descriptor(copy, copy.landing).wait_send()


COPIES = 2 + 8 + 64 + 64


def frozen_block(tokens, gate, up, down):
    hbm = pl.BlockSpec(memory_space=pl.ANY)
    return pl.pallas_call(
        kernel,
        out_shape=jax.ShapeDtypeStruct((128, 4096), F32),
        in_specs=[hbm] * 4,
        out_specs=pl.BlockSpec(memory_space=pltpu.VMEM),
        scratch_shapes=[
            pltpu.VMEM((4, 2, 128, 4096), BF),
            pltpu.VMEM((4096, 896), BF),
            pltpu.VMEM((16, 2, 128, 896), BF),
            pltpu.VMEM((16, 2, 896, 128), BF),
            pltpu.VMEM((4, 256, 896), F32),
            pltpu.VMEM((256, 896), F32),
            pltpu.VMEM((4, 256, 896), BF),
            pltpu.VMEM((16, 4, 128, 256), BF),
            pltpu.VMEM((16, 4, 128, 256), BF),
            pltpu.VMEM((16, 4, 128, 256), BF),
            pltpu.VMEM((8, 128, 256), BF),
            pltpu.VMEM((8, 128, 256), BF),
            pltpu.VMEM((16, 128, 256), BF),
            pltpu.VMEM((16, 128, 256), BF),
            pltpu.SemaphoreType.DMA((4,)),
            pltpu.SemaphoreType.DMA((COPIES,)),
            pltpu.SemaphoreType.DMA((COPIES,)),
        ],
        compiler_params=pltpu.CompilerParams(
            collective_id=0, has_side_effects=True, vmem_limit_bytes=60 * 1024 * 1024),
        cost_estimate=pl.CostEstimate(flops=22_500_000_000, bytes_accessed=16_000_000, transcendentals=1_000_000),
        name="frozen_block",
    )(tokens, gate, up, down)


def shards(
    tokens,
    gate_projection_weight,
    up_projection_weight,
    down_projection_weight,
    router_projection_weight,
    adapter_down_factors,
    adapter_up_factors,
    routes,
    padding_token_mask,
    cotangent,
):
    expert_list = router_projection_weight.shape[1]
    rank_index = adapter_down_factors.shape[1] // expert_list
    logits = jnp.dot(tokens, router_projection_weight, preferred_element_type=F32)
    experts_iota = jnp.arange(expert_list, dtype=jnp.int32)[None, :]
    first_hot = (routes[:, 0:1] == experts_iota).astype(F32)
    second_hot = (routes[:, 1:2] == experts_iota).astype(F32)
    first_logit = jnp.sum(logits * first_hot, axis=1, keepdims=True)
    second_logit = jnp.sum(logits * second_hot, axis=1, keepdims=True)
    weight_first = jax.nn.sigmoid(first_logit - second_logit)
    coeff = weight_first * first_hot + (1.0 - weight_first) * second_hot
    coeff_wide = jnp.repeat(coeff, rank_index, axis=1)
    low_rank_state = jnp.dot(tokens, adapter_down_factors, preferred_element_type=F32)
    scaled_output = (low_rank_state * coeff_wide).astype(BF)
    masked_tokens = cotangent * padding_token_mask[:, None].astype(BF)
    low_rank_gradient = lax.dot_general(
        masked_tokens, adapter_up_factors, (((1,), (1,)), ((), ())), preferred_element_type=F32)
    dlow = (low_rank_gradient * coeff_wide).astype(BF)
    local_live = jnp.sum(padding_token_mask.astype(F32))
    local_up = lax.dot_general(
        scaled_output, masked_tokens, (((0,), (0,)), ((), ())), preferred_element_type=F32)
    local_down = lax.dot_general(
        dlow, tokens, (((0,), (0,)), ((), ())), preferred_element_type=F32)
    packed = jnp.concatenate([local_down, local_up, jnp.full((8, 4096), local_live, F32)], axis=0)
    packed = lax.psum(packed, ("dp", "blk"))
    base = frozen_block(tokens, gate_projection_weight, up_projection_weight, down_projection_weight)
    adapter_delta = jnp.dot(scaled_output, adapter_up_factors, preferred_element_type=F32)
    layer_out = (base + adapter_delta).astype(BF)
    inverse = 1.0 / jnp.maximum(packed[256, 0], 1.0)
    grad_down = packed[:128].T * inverse
    grad_up = packed[128:256] * inverse
    return (layer_out, grad_down, grad_up)


def solution(mesh):
    return jax.shard_map(
        shards,
        mesh=mesh,
        in_specs=(
            P(("dp", "blk"), None),
            P(None, "blk"),
            P("dp", "blk"),
            P("blk", "dp"),
            P(),
            P(),
            P(),
            P(("dp", "blk"), None),
            P(("dp", "blk")),
            P(("dp", "blk"), None),
        ),
        out_specs=(P(("dp", "blk"), None), P(), P()),
        check_vma=False,
    )
```

```python
import jax
import jax.numpy as jnp
from jax import lax
from jax.experimental import pallas as pl
from jax.experimental.pallas import tpu as pltpu
from jax.sharding import PartitionSpec as P

MESH = pl.DeviceIdType.MESH
BF, F32 = jnp.bfloat16, jnp.float32

REL = (0, 1, 3, 2)
LINK_RATE, PAIR_RATE = 46.6e3, 300e3
HOP, PAIR_HOP = 1.8, 1.0
AHEAD = 1.5
GRAD_RANK = 50


class Copy:
    def __init__(self, name, link, size, source, landing, here, rank):
        self.name, self.link, self.size, self.rank = name, link, size, rank
        self.source, self.landing, self.here = source, landing, here
        self.after = set()


class Task:
    def __init__(self, name, cost, run, after, rank):
        self.name, self.cost, self.run, self.after, self.rank = name, cost, run, set(after), rank


def arrange(copies, tasks, begun):
    order, done, now = [], set(begun), 0.0
    free, arriving, queued = {}, [], {}
    to_send, to_run = list(copies), list(tasks)

    def send(copy):
        order.append(("send", copy))
        rate, hop = (PAIR_RATE, PAIR_HOP) if copy.link == "pair" else (LINK_RATE, HOP)
        start = max(now, free.get(copy.link, 0.0))
        free[copy.link] = end = start + copy.size / rate
        arriving.append((end + hop, copy))

    def send_ready(until):
        for copy in list(to_send):
            if copy.after <= done:
                to_send.remove(copy)
                queued.setdefault(copy.link, []).append(copy)
        for link, line in queued.items():
            line.sort(key=lambda copy: copy.rank)
            while line and (free.get(link, 0.0) < until or link == "pair"):
                send(line.pop(0))

    send_ready(AHEAD)
    while arriving or to_run:
        arriving.sort(key=lambda pair: pair[0])
        ready = [task for task in to_run if task.after <= done]
        if arriving and arriving[0][0] <= now:
            copy = arriving.pop(0)[1]
            order.append(("recv", copy))
            done.add(copy.name)
            send_ready(now + AHEAD)
        elif ready:
            task = min(ready, key=lambda task: task.rank)
            to_run.remove(task)
            order.append(("task", task))
            now += task.cost
            done.add(task.name)
            send_ready(now + AHEAD)
        else:
            send_ready(arriving[0][0] + AHEAD)
            arriving.sort(key=lambda pair: pair[0])
            now = arriving[0][0]
    assert not to_send
    return order, now


def kernel(tokens, gate, up, down, grad_low, grad_high, live, base, grads, tok, gw, ub, db, gact, uact, hid, psib, rsib, summed,
           rl, rr, fl, fr, ustage, dstage, g, own, live_pair, rz, rm, xs, ga, gb, load_sem, send_sem, recv_sem):
    dp, blk = lax.axis_index("dp"), lax.axis_index("blk")
    z, y, xh = dp // 8, (dp // 2) % 4, dp % 2
    xl, core = blk // 2, blk % 2
    x = xh * 2 + xl

    def device(dz=0, dy=0, dx=0, dc=0):
        at_z, at_y, at_x = (z + dz) % 4, (y + dy) % 4, (x + dx) % 4
        return ((at_z * 4 + at_y) * 2 + at_x // 2, (at_x % 2) * 2 + (core + dc) % 2)

    targets = {
        "z+": device(dz=1), "z-": device(dz=3), "y+": device(dy=1), "y-": device(dy=3),
        "x+": device(dx=1), "x-": device(dx=3), "pair": device(dc=1),
    }

    def plane(dz, dy):
        return ((z + dz) % 4) * 4 + (y + dy) % 4

    copies = []

    def add(name, link, size, source, landing, here, after=(), rank=0):
        copy = Copy(name, link, size, source, landing, here, rank)
        copy.after = set(after)
        copies.append(copy)
        return copy

    piece = 128 * 896 * 2

    def weight(kind, dz, dy, own, half=None):
        ref, rows = (ub, 128) if kind == "u" else (db, 896)
        ref = ref.at[plane(dz, dy), xh if own else 1 - xh]
        if half is None:
            return ref
        return ref.at[pl.ds(half * (rows // 2), rows // 2)]

    def spread(tag, ref, size, first, origin, base_rank):
        second = "z" if first == "y" else "y"

        def at(f, s, half=None):
            return ref(f, s, half) if first == "z" else ref(s, f, half)

        def move(name, link, f, s, f_new, s_new, after, rank, half=None):
            amount = size if half is None else size // 2
            add(tag + name, link, amount, at(f, s, half), at(f, s, half), at(f_new, s_new, half), after, rank + base_rank)

        move("F+", first + "+", 0, 0, 3, 0, origin, 0)
        move("F-", first + "-", 0, 0, 1, 0, origin, 0)
        move("S+0", second + "+", 0, 0, 0, 3, origin, 1)
        move("S-0", second + "-", 0, 0, 0, 1, origin, 1)
        move("G+", first + "+", 3, 0, 2, 0, [tag + "F+"], 2, 0)
        move("G-", first + "-", 1, 0, 2, 0, [tag + "F-"], 2, 1)
        came = {0: origin, 3: [tag + "F+"], 1: [tag + "F-"], 2: [tag + "G+", tag + "G-"]}
        for f in REL[1:]:
            move("S+%d" % f, second + "+", f, 0, f, 3, came[f], 4 if f == 2 else 3)
            move("S-%d" % f, second + "-", f, 0, f, 1, came[f], 4 if f == 2 else 3)
        for f in (0, 1):
            move("T+%d" % f, second + "+", f, 3, f, 2, [tag + "S+%d" % f], 5)
        for f in (3, 2):
            move("T-%d" % f, second + "-", f, 1, f, 2, [tag + "S-%d" % f], 5)

        def have(f, s):
            if s == 0:
                return came[f]
            if s == 3:
                return [tag + "S+%d" % f]
            if s == 1:
                return [tag + "S-%d" % f]
            return [tag + ("T+%d" if f in (0, 1) else "T-%d") % f]

        return (lambda dz, dy: have(dz, dy)) if first == "z" else (lambda dz, dy: have(dy, dz))

    def across(kind, hbm, ref, stage, rows, rank):
        for sign, step, half in (("+", 1, 0), ("-", 3, 1)):
            part = pl.ds(half * rows, rows)
            if kind == "u":
                source = hbm.at[part, pl.ds(pl.multiple_of((1 - xh) * 896, 128), 896)]
            else:
                source = hbm.at[pl.ds(pl.multiple_of((1 - xh) * 896 + half * rows, 64), rows), :]
            next_half = 1 - ((x + step) % 4) // 2
            hold = stage.at[half]
            add("A" + kind + sign, "x" + sign, piece // 2, source, hold, hold, [], rank)
            add("B" + kind + sign, "x" + sign, piece // 2, hold, ref.at[plane(0, 0), next_half, part],
                ref.at[plane(0, 0), 1 - xh, part], ["A" + kind + sign], rank)
        return ["B" + kind + "+", "B" + kind + "-"]

    mib = 128 * 4096 * 2
    have_au = across("u", up, ub, ustage, 64, 0)
    quarters = [pl.ds(32 * q, 32) for q in range(4)]
    for sign, r, order4 in (("+", 3, (0, 1, 2, 3)), ("-", 1, (2, 3, 0, 1))):
        for n, q in enumerate(order4):
            part = quarters[q]
            add("K%s%d" % (sign, q), "x" + sign, mib // 4, tok.at[0, 0, part], tok.at[r, 0, part], tok.at[r, 0, part], ["L", "Au" + sign], 3)
            if n < 2:
                add("KF%d" % q, "x" + sign, mib // 4, tok.at[r, 0, part], tok.at[2, 0, part], tok.at[2, 0, part], ["K%s%d" % (sign, q)], 4)
                add("KP%d" % q, "pair", mib // 4, tok.at[2, 0, part], tok.at[2, 1, part], tok.at[2, 1, part], ["KF%d" % q])
    came_near = {0: ["L"], 3: ["K+%d" % q for q in range(4)], 1: ["K-%d" % q for q in range(4)]}
    for r in (0, 1, 3):
        add("KS%d" % r, "pair", mib, tok.at[r, 0], tok.at[r, 1], tok.at[r, 1], came_near[r])
    came_near[2] = ["KF%d" % q for q in range(4)]
    came_pair = {r: ["KS%d" % r] for r in (0, 1, 3)}
    came_pair[2] = ["KP%d" % q for q in range(4)]
    have_ad = across("d", down, db, dstage, 448, 5)
    def piece_of(kind, own):
        return lambda dz, dy, half: weight(kind, dz, dy, own, half)

    have_uo = spread("uo", piece_of("u", True), piece, "y", ["L"], 0)
    have_up = spread("up", piece_of("u", False), piece, "z", have_au, 0)
    have_do = spread("do", piece_of("d", True), piece, "z", ["L"], 100)
    have_dp = spread("dp", piece_of("d", False), piece, "y", have_ad, 100)
    came_tok = {r: came_near[r] + came_pair[r] for r in REL}

    tasks = []

    def run_gate(places):
        def run():
            def step(i, carry):
                k = pl.multiple_of(i * 512, 512)
                left = jnp.concatenate([tok[r, :, :, pl.ds(k, 512)].reshape(256, 512) for r in places], axis=0)
                part = jnp.dot(left, gw[pl.ds(k, 512), :], preferred_element_type=F32)
                for n, r in enumerate(places):
                    uact[r] += part[n * 256:n * 256 + 256]
                return carry

            for r in places:
                uact[r] = jnp.zeros((256, 896), F32)
            lax.fori_loop(0, 8, step, 0)
            for r in places:
                v = uact[r]
                gact[r] = v / (1.0 + jnp.exp(-v))
                uact[r] = jnp.zeros((256, 896), F32)
        return run

    def run_up(dz, dy, i):
        def run():
            j = plane(dz, dy)
            columns = pl.ds(pl.multiple_of(j * 256, 256), 256)
            two = pl.ds(i * 2, 2)
            left = tok[two, :, :, columns].reshape(512, 256)
            part = jnp.dot(left, ub[j].reshape(256, 896), preferred_element_type=F32)
            uact[two] += part.reshape(2, 256, 896)
        return run

    def run_hidden():
        hid[...] = (gact[...] * uact[...]).astype(BF)

    ups = []
    for name, cost, places in (("G0", 5.7, (0,)), ("G1", 9.0, (1, 3)), ("G2", 5.7, (2,))):
        tasks.append(Task(name, cost, run_gate(places), [n for r in places for n in came_tok[r]] + ["LG"], 10))
    for dz in range(4):
        for dy in range(4):
            for i in (0, 1):
                ups.append("U%d%d%d" % (dz, dy, i))
                ready = have_uo(dz, dy) + have_up(dz, dy) + ["G1", "G2" if i else "G0"]
                tasks.append(Task(ups[-1], 0.45, run_up(dz, dy, i), ready, 20 + i))
    tasks.append(Task("H", 0.5, run_hidden, ups, 0))
    blocks = sorted(((dz, dy) for dz in range(4) for dy in range(4)), key=lambda p: (min(p[0], 4 - p[0]) + min(p[1], 4 - p[1]), p))
    size = 128 * 256 * 2

    slot = {}

    def run_down(b, dz, dy):
        def run():
            j = plane(dz, dy)
            right = jnp.concatenate([db[j, 0], db[j, 1]], axis=1)

            def step(i, carry):
                left = hid[pl.ds(i * 2, 2)].reshape(512, 896)
                part = jnp.dot(left, right, preferred_element_type=F32).astype(BF).reshape(2, 2, 128, 256)
                summed[b, pl.ds(i * 2, 2)] = part[:, 0]
                psib[slot[b], pl.ds(i * 2, 2)] = part[:, 1]
                return carry

            lax.fori_loop(0, 2, step, 0)
        return run

    def run_add(b):
        def run():
            summed[b] = (summed[b].astype(F32) + rsib[b].astype(F32)).astype(BF)
        return run

    def run_merge(b):
        def run():
            if b % 2 == 0:
                summed[b, 1] = (summed[b, 1].astype(F32) + rl[b // 2].astype(F32)).astype(BF)
            else:
                summed[b, 3] = (summed[b, 3].astype(F32) + rr[b // 2].astype(F32)).astype(BF)
        return run

    def run_final(b, dz, dy):
        def run():
            total = summed[b, 0].astype(F32) + fl[b].astype(F32) + fr[b].astype(F32)
            base[:, pl.ds(pl.multiple_of(plane(dz, dy) * 256, 256), 256)] = total
        return run

    hidden = ["H"]
    for b, (dz, dy) in enumerate(blocks):
        n, half = str(b), b // 2
        tasks.append(Task("D" + n, 1.25, run_down(b, dz, dy), hidden + have_do(dz, dy) + have_dp(dz, dy), 300 + b))
        add("Q" + n, "pair", 4 * size, None, rsib.at[b], rsib.at[b], ["D" + n])
        tasks.append(Task("A" + n, 0.15, run_add(b), ["D" + n, "Q" + n], 200 + b))
        if b % 2 == 0:
            add("Z" + n, "x+", size, summed.at[b, 2], rl.at[half], rl.at[half], ["A" + n], 10 + 3 * b)
            add("N" + n, "x-", size, summed.at[b, 3], fr.at[b], fr.at[b], ["A" + n], 12 + 3 * b)
            add("M" + n, "x+", size, summed.at[b, 1], fl.at[b], fl.at[b], ["C" + n], 11 + 3 * b)
        else:
            add("Z" + n, "x-", size, summed.at[b, 2], rr.at[half], rr.at[half], ["A" + n], 10 + 3 * b)
            add("N" + n, "x+", size, summed.at[b, 1], fl.at[b], fl.at[b], ["A" + n], 12 + 3 * b)
            add("M" + n, "x-", size, summed.at[b, 3], fr.at[b], fr.at[b], ["C" + n], 11 + 3 * b)
        tasks.append(Task("C" + n, 0.05, run_merge(b), ["A" + n, "Z" + n], 100 + b))
        tasks.append(Task("E" + n, 0.1, run_final(b, dz, dy), ["A" + n, "M" + n, "N" + n], 400 + b))

    wide = 1152 * 4
    pair_after = ["PL"]
    add("PL", "pair", 4096, live, live_pair, live_pair, [], 0)
    for ab in range(2):
        there = pl.ds(pl.multiple_of((1 - core) * 2048 + ab * 1024, 1024), 1024)
        for h, part in enumerate((grad_low, grad_high)):
            landing = g.at[ab, pl.ds(h * 128, 128), pl.ds(0, 1024)]
            add("PG%d%d" % (ab, h), "pair", 128 * 4096, part.at[:, there], landing, landing, [], 1)
            pair_after.append("PG%d%d" % (ab, h))

    def run_own():
        parts = [(ab, h, n) for ab in range(2) for h in range(2) for n in range(2)]

        def fetch(i):
            ab, h, n = parts[i]
            here = pl.ds(pl.multiple_of(core * 2048 + ab * 1024, 1024), 1024)
            part = (grad_low, grad_high)[h]
            return pltpu.make_async_copy(part.at[pl.ds(n * 64, 64), here], own.at[i % 2], load_sem.at[4 + i % 2])

        fetch(0).start()
        for i, (ab, h, n) in enumerate(parts):
            if i + 1 < len(parts):
                fetch(i + 1).start()
            fetch(i).wait()
            g[ab, h * 128 + n * 64:h * 128 + n * 64 + 64, 0:1024] += own[i % 2]
        count = live[0:1, :] + live_pair[0:1, :]
        for ab in range(2):
            g[ab, :, 1024:1152] = jnp.broadcast_to(count, (256, 128))

    tasks.append(Task("PA", 6.0, run_own, pair_after, 5))

    def reduce_ring(tag, axis, piece_at, hold_z, hold_m, rows, after, finish, rank):
        amount = rows * wide
        for sign, near, half in (("+", 1, 0), ("-", 3, 1)):
            add(tag + "Z" + sign, axis + sign, amount // 2, piece_at(2, half), hold_z.at[half], hold_z.at[half], after, rank)

            def combine(near=near, half=half):
                ref = piece_at(near, half)
                ref[...] = ref[...] + hold_z[half]

            tasks.append(Task(tag + "C" + sign, 0.2, combine, after + [tag + "Z" + sign], 6))
            add(tag + "M" + sign, axis + sign, amount, piece_at(near), hold_m.at[half], hold_m.at[half], [tag + "C" + sign], rank)
        tasks.append(Task(tag + "E", 0.3, finish, after + [tag + "M+", tag + "M-"], 6))

    row_of = {"y": y, "z": z}
    for ab, (first, second) in enumerate((("y", "z"), ("z", "y"))):
        p, q = row_of[first], row_of[second]

        def block(d, half=None, ab=ab, p=p):
            rows = pl.multiple_of(((p + d) % 4) * 64 + (half or 0) * 32, 32)
            return g.at[ab, pl.ds(rows, 64 if half is None else 32)]

        def small(d, half=None, ab=ab, p=p, q=q):
            rows = pl.multiple_of(p * 64 + ((q + d) % 4) * 16 + (half or 0) * 8, 8)
            return g.at[ab, pl.ds(rows, 16 if half is None else 8)]

        z1, m1 = rz.at[ab, :, pl.ds(0, 32)], rm.at[ab, :, pl.ds(0, 64)]
        z2, m2 = rz.at[ab, :, pl.ds(32, 8)], rm.at[ab, :, pl.ds(64, 16)]

        def first_done(block=block, ab=ab):
            ref = block(0)
            ref[...] = ref[...] + rm[ab, 0, 0:64] + rm[ab, 1, 0:64]

        def second_done(small=small, ab=ab):
            xs[0, ab] = small(0)[...] + rm[ab, 0, 64:80] + rm[ab, 1, 64:80]

        reduce_ring("R%d" % ab, first, block, z1, m1, 64, ["PA"], first_done, GRAD_RANK)
        reduce_ring("S%d" % ab, second, small, z2, m2, 16, ["R%dE" % ab], second_done, GRAD_RANK)

    slices = ["S0E", "S1E"]
    add("X+", "x+", 32 * wide, xs.at[0], xs.at[3], xs.at[3], slices, 6)
    add("X-", "x-", 32 * wide, xs.at[0], xs.at[1], xs.at[1], slices, 6)
    add("XF+", "x+", 16 * wide, xs.at[3, 0], xs.at[2, 0], xs.at[2, 0], ["X+"], 6)
    add("XF-", "x-", 16 * wide, xs.at[1, 1], xs.at[2, 1], xs.at[2, 1], ["X-"], 6)

    def row_block(ab, dz, dy):
        at_z, at_y = (z + dz) % 4, (y + dy) % 4
        return at_z * 4 + at_y if ab else at_y * 4 + at_z

    def run_whole():
        for ab in range(2):
            total = (xs[0, ab] + xs[2, ab]) + (xs[1, ab] + xs[3, ab])
            inverse = 1.0 / jnp.maximum(total[:, 1024:1025], 1.0)
            ga[ab, row_block(ab, 0, 0)] = (total[:, 0:1024] * inverse).astype(BF)

    tasks.append(Task("XS", 0.4, run_whole, slices + ["X+", "X-", "XF+", "XF-"], 6))
    for ab, first in enumerate("yz"):
        def finished(dz, dy, half, ab=ab):
            ref = ga.at[ab, row_block(ab, dz, dy)]
            return ref if half is None else ref.at[:, pl.ds(half * 512, 512)]

        have = spread("g%d" % ab, finished, 16 * 1024 * 2, first, ["XS"], GRAD_RANK)
        whole = sorted({n for dz in range(4) for dy in range(4) for n in have(dz, dy)})
        add("PH%d" % ab, "pair", 256 * 1024 * 2, ga.at[ab], gb.at[ab], gb.at[ab], whole)

    order, _ = arrange(copies, tasks, ["L", "LG"])
    assert len(copies) == COPIES
    place = {copy.name: i for i, copy in enumerate(copies)}
    by_name = {copy.name: copy for copy in copies}

    def descriptor(copy, landing):
        i = place[copy.name]
        return pltpu.make_async_remote_copy(
            src_ref=copy.source, dst_ref=landing, send_sem=send_sem.at[i], recv_sem=recv_sem.at[i],
            device_id=targets[copy.link], device_id_type=MESH)

    loads = [
        pltpu.make_async_copy(tokens, tok.at[0, 0], load_sem.at[0]),
        pltpu.make_async_copy(up.at[:, pl.ds(pl.multiple_of(xh * 896, 128), 896)], ub.at[plane(0, 0), xh], load_sem.at[1]),
        pltpu.make_async_copy(down.at[pl.ds(pl.multiple_of(xh * 896, 128), 896), :], db.at[plane(0, 0), xh], load_sem.at[2]),
    ]
    load_gate = pltpu.make_async_copy(gate.at[:, pl.ds(pl.multiple_of(xh * 896, 128), 896)], gw, load_sem.at[3])
    for load in loads:
        load.start()
    load_gate.start()
    barrier = pltpu.get_barrier_semaphore()
    for target in targets.values():
        pl.semaphore_signal(barrier, inc=1, device_id=target, device_id_type=MESH)
    pl.semaphore_wait(barrier, len(targets))
    for load in loads:
        load.wait()
    gate_waited = False
    used = []
    for what, item in order:
        if item.name[0] == "D" and what == "task":
            if len(used) >= 8:
                early = by_name["Q" + used[-8]]
                descriptor(early, early.landing).wait_send()
            slot[int(item.name[1:])] = len(used) % 8
            used.append(item.name[1:])
            by_name["Q" + used[-1]].source = psib.at[slot[int(used[-1])]]
        if what == "send":
            descriptor(item, item.landing).start()
        elif what == "recv":
            descriptor(item, item.here).wait_recv()
        else:
            if item.name[0] == "G" and not gate_waited:
                load_gate.wait()
                gate_waited = True
            item.run()
    stores = [pltpu.make_async_copy(ga, grads.at[core], load_sem.at[4]), pltpu.make_async_copy(gb, grads.at[1 - core], load_sem.at[5])]
    for store in stores:
        store.start()
    already = {"Q" + n for n in used[:-8]}
    for copy in copies:
        if copy.name not in already:
            descriptor(copy, copy.landing).wait_send()
    for store in stores:
        store.wait()


COPIES = 8 + 19 + 64 + 64 + 5 + 16 + 4 + 32 + 2


def frozen_block(tokens, gate, up, down, grad_low, grad_high, live):
    hbm = pl.BlockSpec(memory_space=pl.ANY)
    return pl.pallas_call(
        kernel,
        out_shape=(jax.ShapeDtypeStruct((128, 4096), F32), jax.ShapeDtypeStruct((2, 2, 16, 16, 1024), BF)),
        in_specs=[hbm] * 6 + [pl.BlockSpec(memory_space=pltpu.VMEM)],
        out_specs=(pl.BlockSpec(memory_space=pltpu.VMEM), hbm),
        scratch_shapes=[
            pltpu.VMEM((4, 2, 128, 4096), BF),
            pltpu.VMEM((4096, 896), BF),
            pltpu.VMEM((16, 2, 128, 896), BF),
            pltpu.VMEM((16, 2, 896, 128), BF),
            pltpu.VMEM((4, 256, 896), F32),
            pltpu.VMEM((4, 256, 896), F32),
            pltpu.VMEM((4, 256, 896), BF),
            pltpu.VMEM((8, 4, 128, 256), BF),
            pltpu.VMEM((16, 4, 128, 256), BF),
            pltpu.VMEM((16, 4, 128, 256), BF),
            pltpu.VMEM((8, 128, 256), BF),
            pltpu.VMEM((8, 128, 256), BF),
            pltpu.VMEM((16, 128, 256), BF),
            pltpu.VMEM((16, 128, 256), BF),
            pltpu.VMEM((2, 64, 896), BF),
            pltpu.VMEM((2, 448, 128), BF),
            pltpu.VMEM((2, 256, 1152), F32),
            pltpu.VMEM((2, 64, 1024), F32),
            pltpu.VMEM((8, 128), F32),
            pltpu.VMEM((2, 2, 40, 1152), F32),
            pltpu.VMEM((2, 2, 80, 1152), F32),
            pltpu.VMEM((4, 2, 16, 1152), F32),
            pltpu.VMEM((2, 16, 16, 1024), BF),
            pltpu.VMEM((2, 16, 16, 1024), BF),
            pltpu.SemaphoreType.DMA((6,)),
            pltpu.SemaphoreType.DMA((COPIES,)),
            pltpu.SemaphoreType.DMA((COPIES,)),
        ],
        compiler_params=pltpu.CompilerParams(
            collective_id=0, has_side_effects=True, vmem_limit_bytes=67_000_000),
        cost_estimate=pl.CostEstimate(flops=22_500_000_000, bytes_accessed=16_000_000, transcendentals=1_000_000),
        name="frozen_block",
    )(tokens, gate, up, down, grad_low, grad_high, live)


def shards(
    tokens,
    gate_projection_weight,
    up_projection_weight,
    down_projection_weight,
    router_projection_weight,
    adapter_down_factors,
    adapter_up_factors,
    routes,
    padding_token_mask,
    cotangent,
):
    expert_list = router_projection_weight.shape[1]
    rank_index = adapter_down_factors.shape[1] // expert_list
    logits = jnp.dot(tokens, router_projection_weight, preferred_element_type=F32)
    experts_iota = jnp.arange(expert_list, dtype=jnp.int32)[None, :]
    first_hot = (routes[:, 0:1] == experts_iota).astype(F32)
    second_hot = (routes[:, 1:2] == experts_iota).astype(F32)
    first_logit = jnp.sum(logits * first_hot, axis=1, keepdims=True)
    second_logit = jnp.sum(logits * second_hot, axis=1, keepdims=True)
    weight_first = jax.nn.sigmoid(first_logit - second_logit)
    coeff = weight_first * first_hot + (1.0 - weight_first) * second_hot
    coeff_wide = jnp.repeat(coeff, rank_index, axis=1)
    low_rank_state = jnp.dot(tokens, adapter_down_factors, preferred_element_type=F32)
    scaled_output = (low_rank_state * coeff_wide).astype(BF)
    masked_tokens = cotangent * padding_token_mask[:, None].astype(BF)
    low_rank_gradient = lax.dot_general(
        masked_tokens, adapter_up_factors, (((1,), (1,)), ((), ())), preferred_element_type=F32)
    dlow = (low_rank_gradient * coeff_wide).astype(BF)
    local_live = jnp.sum(padding_token_mask.astype(F32))
    local_up = lax.dot_general(
        scaled_output, masked_tokens, (((0,), (0,)), ((), ())), preferred_element_type=F32)
    local_down = lax.dot_general(
        dlow, tokens, (((0,), (0,)), ((), ())), preferred_element_type=F32)
    base, grads = frozen_block(
        tokens, gate_projection_weight, up_projection_weight, down_projection_weight,
        local_down, local_up, jnp.full((8, 128), local_live, F32))
    adapter_delta = jnp.dot(scaled_output, adapter_up_factors, preferred_element_type=F32)
    layer_out = (base + adapter_delta).astype(BF)
    rows = grads.reshape(2, 2, 256, 1024)
    grad_down = rows[:, :, :128].transpose(0, 1, 3, 2).reshape(4096, 128).astype(F32)
    grad_up = rows[:, :, 128:].transpose(2, 0, 1, 3).reshape(128, 4096).astype(F32)
    return (layer_out, grad_down, grad_up)


def solution(mesh):
    return jax.shard_map(
        shards,
        mesh=mesh,
        in_specs=(
            P(("dp", "blk"), None),
            P(None, "blk"),
            P("dp", "blk"),
            P("blk", "dp"),
            P(),
            P(),
            P(),
            P(("dp", "blk"), None),
            P(("dp", "blk")),
            P(("dp", "blk"), None),
        ),
        out_specs=(P(("dp", "blk"), None), P(), P()),
        check_vma=False,
    )
```

```python
import jax
import jax.numpy as jnp
from jax import lax
from jax.experimental import pallas as pl
from jax.experimental.pallas import tpu as pltpu
from jax.sharding import PartitionSpec as P

MESH = pl.DeviceIdType.MESH
BF, F32 = jnp.bfloat16, jnp.float32

REL = (0, 1, 3, 2)
LINK_RATE, PAIR_RATE = 46.6e3, 300e3
HOP, PAIR_HOP = 1.8, 1.0
AHEAD = 1.5
GRAD_RANK = 50
SLOTS = 3


class Copy:
    def __init__(self, name, link, size, source, landing, here, rank):
        self.name, self.link, self.size, self.rank = name, link, size, rank
        self.source, self.landing, self.here = source, landing, here
        self.after = set()


class Task:
    def __init__(self, name, cost, run, after, rank):
        self.name, self.cost, self.run, self.after, self.rank = name, cost, run, set(after), rank


def arrange(copies, tasks, begun):
    order, done, now = [], set(begun), 0.0
    free, arriving, queued = {}, [], {}
    to_send, to_run = list(copies), list(tasks)

    def send(copy):
        order.append(("send", copy))
        rate, hop = (PAIR_RATE, PAIR_HOP) if copy.link == "pair" else (LINK_RATE, HOP)
        start = max(now, free.get(copy.link, 0.0))
        free[copy.link] = end = start + copy.size / rate
        arriving.append((end + hop, copy))

    def send_ready(until):
        for copy in list(to_send):
            if copy.after <= done:
                to_send.remove(copy)
                queued.setdefault(copy.link, []).append(copy)
        for link, line in queued.items():
            line.sort(key=lambda copy: copy.rank)
            while line and (free.get(link, 0.0) < until or link == "pair"):
                send(line.pop(0))

    send_ready(AHEAD)
    while arriving or to_run:
        arriving.sort(key=lambda pair: pair[0])
        ready = [task for task in to_run if task.after <= done]
        if arriving and arriving[0][0] <= now:
            copy = arriving.pop(0)[1]
            order.append(("recv", copy))
            done.add(copy.name)
            send_ready(now + AHEAD)
        elif ready:
            task = min(ready, key=lambda task: task.rank)
            to_run.remove(task)
            order.append(("task", task))
            now += task.cost
            done.add(task.name)
            send_ready(now + AHEAD)
        else:
            send_ready(arriving[0][0] + AHEAD)
            arriving.sort(key=lambda pair: pair[0])
            now = arriving[0][0]
    assert not to_send
    return order, now


def kernel(tokens, gate, up, down, cotangent, factors_down, factors_up, router, small, base, grads, tok, gw, ub, db, gact, uact, hid, psib, rsib, summed,
           rl, rr, fl, fr, ustage, dstage, g, stage, cot, fdown, fup, coef, scaled, turned, rz, rm, xs, ga, gb, load_sem, send_sem, recv_sem):
    dp, blk = lax.axis_index("dp"), lax.axis_index("blk")
    z, y, xh = dp // 8, (dp // 2) % 4, dp % 2
    xl, core = blk // 2, blk % 2
    x = xh * 2 + xl

    def device(dz=0, dy=0, dx=0, dc=0):
        at_z, at_y, at_x = (z + dz) % 4, (y + dy) % 4, (x + dx) % 4
        return ((at_z * 4 + at_y) * 2 + at_x // 2, (at_x % 2) * 2 + (core + dc) % 2)

    targets = {
        "z+": device(dz=1), "z-": device(dz=3), "y+": device(dy=1), "y-": device(dy=3),
        "x+": device(dx=1), "x-": device(dx=3), "pair": device(dc=1),
    }

    def plane(dz, dy):
        return ((z + dz) % 4) * 4 + (y + dy) % 4

    copies = []

    def add(name, link, size, source, landing, here, after=(), rank=0):
        copy = Copy(name, link, size, source, landing, here, rank)
        copy.after = set(after)
        copies.append(copy)
        return copy

    piece = 128 * 896 * 2

    def weight(kind, dz, dy, own, half=None):
        ref, rows = (ub, 128) if kind == "u" else (db, 896)
        ref = ref.at[plane(dz, dy), xh if own else 1 - xh]
        if half is None:
            return ref
        return ref.at[pl.ds(half * (rows // 2), rows // 2)]

    def spread(tag, ref, size, first, origin, base_rank):
        second = "z" if first == "y" else "y"

        def at(f, s, half=None):
            return ref(f, s, half) if first == "z" else ref(s, f, half)

        def move(name, link, f, s, f_new, s_new, after, rank, half=None):
            amount = size if half is None else size // 2
            add(tag + name, link, amount, at(f, s, half), at(f, s, half), at(f_new, s_new, half), after, rank + base_rank)

        move("F+", first + "+", 0, 0, 3, 0, origin, 0)
        move("F-", first + "-", 0, 0, 1, 0, origin, 0)
        move("S+0", second + "+", 0, 0, 0, 3, origin, 1)
        move("S-0", second + "-", 0, 0, 0, 1, origin, 1)
        move("G+", first + "+", 3, 0, 2, 0, [tag + "F+"], 2, 0)
        move("G-", first + "-", 1, 0, 2, 0, [tag + "F-"], 2, 1)
        came = {0: origin, 3: [tag + "F+"], 1: [tag + "F-"], 2: [tag + "G+", tag + "G-"]}
        for f in REL[1:]:
            move("S+%d" % f, second + "+", f, 0, f, 3, came[f], 4 if f == 2 else 3)
            move("S-%d" % f, second + "-", f, 0, f, 1, came[f], 4 if f == 2 else 3)
        for f in (0, 1):
            move("T+%d" % f, second + "+", f, 3, f, 2, [tag + "S+%d" % f], 5)
        for f in (3, 2):
            move("T-%d" % f, second + "-", f, 1, f, 2, [tag + "S-%d" % f], 5)

        def have(f, s):
            if s == 0:
                return came[f]
            if s == 3:
                return [tag + "S+%d" % f]
            if s == 1:
                return [tag + "S-%d" % f]
            return [tag + ("T+%d" if f in (0, 1) else "T-%d") % f]

        return (lambda dz, dy: have(dz, dy)) if first == "z" else (lambda dz, dy: have(dy, dz))

    def across(kind, hbm, ref, stage, rows, rank):
        for sign, step, half in (("+", 1, 0), ("-", 3, 1)):
            part = pl.ds(half * rows, rows)
            if kind == "u":
                source = hbm.at[part, pl.ds(pl.multiple_of((1 - xh) * 896, 128), 896)]
            else:
                source = hbm.at[pl.ds(pl.multiple_of((1 - xh) * 896 + half * rows, 64), rows), :]
            next_half = 1 - ((x + step) % 4) // 2
            hold = stage.at[half]
            add("A" + kind + sign, "x" + sign, piece // 2, source, hold, hold, [], rank)
            add("B" + kind + sign, "x" + sign, piece // 2, hold, ref.at[plane(0, 0), next_half, part],
                ref.at[plane(0, 0), 1 - xh, part], ["A" + kind + sign], rank)
        return ["B" + kind + "+", "B" + kind + "-"]

    mib = 128 * 4096 * 2
    have_au = across("u", up, ub, ustage, 64, 0)
    def columns_of(dz):
        return pl.ds(pl.multiple_of(((z + dz) % 4) * 1024, 1024), 1024)

    def some(r, c, dz):
        return tok.at[r, c, :, columns_of(dz)]

    came_tok = {}
    for dz in REL:
        came_tok[0, dz] = ["L"]
        for sign, r in (("+", 3), ("-", 1)):
            add("K%s%d" % (sign, dz), "x" + sign, mib // 4, some(0, 0, dz), some(r, 0, dz), some(r, 0, dz), ["L", "Au" + sign], 3)
            came_tok[r, dz] = ["K%s%d" % (sign, dz)]
        sign, r = ("+", 3) if dz < 2 else ("-", 1)
        add("KF%d" % dz, "x" + sign, mib // 4, some(r, 0, dz), some(2, 0, dz), some(2, 0, dz), came_tok[r, dz], 4)
        came_tok[2, dz] = ["KF%d" % dz]
        for r in REL:
            add("KS%d%d" % (r, dz), "pair", mib // 4, some(r, 0, dz), some(r, 1, dz), some(r, 1, dz), came_tok[r, dz])
            came_tok[r, dz] = came_tok[r, dz] + ["KS%d%d" % (r, dz)]
    have_ad = across("d", down, db, dstage, 448, 5)
    def piece_of(kind, own):
        return lambda dz, dy, half: weight(kind, dz, dy, own, half)

    have_uo = spread("uo", piece_of("u", True), piece, "y", ["L"], 0)
    have_up = spread("up", piece_of("u", False), piece, "z", have_au, 0)
    have_do = spread("do", piece_of("d", True), piece, "z", ["L"], 100)
    have_dp = spread("dp", piece_of("d", False), piece, "y", have_ad, 100)

    tasks = []

    def run_gate(places, n, dz):
        def run():
            def step(i, carry):
                k = pl.multiple_of(((z + dz) % 4) * 1024 + i * 512, 512)
                left = jnp.concatenate([tok[r, :, :, pl.ds(k, 512)].reshape(256, 512) for r in places], axis=0)
                part = jnp.dot(left, gw[pl.ds(k, 512), :], preferred_element_type=F32)
                for m, r in enumerate(places):
                    gact[r] += part[m * 256:m * 256 + 256]
                return carry

            if n == 0:
                for r in places:
                    gact[r] = jnp.zeros((256, 896), F32)
                    uact[r] = jnp.zeros((256, 896), F32)
            lax.fori_loop(0, 2, step, 0)
            if n == 3:
                for r in places:
                    v = gact[r]
                    gact[r] = v / (1.0 + jnp.exp(-v))
        return run

    def run_up(dz, dy, i):
        def run():
            j = plane(dz, dy)
            columns = pl.ds(pl.multiple_of(j * 256, 256), 256)
            two = pl.ds(i * 2, 2)
            left = tok[two, :, :, columns].reshape(512, 256)
            part = jnp.dot(left, ub[j].reshape(256, 896), preferred_element_type=F32)
            uact[two] += part.reshape(2, 256, 896)
        return run

    def run_hidden():
        hid[...] = (gact[...] * uact[...]).astype(BF)

    ups = []
    for name, cost, places in (("G0", 1.4, (0,)), ("G1", 2.2, (1, 3)), ("G2", 1.4, (2,))):
        for n, dz in enumerate(REL):
            ready = [name + str(n - 1)] if n else ["LG"]
            tasks.append(Task(name + str(n), cost, run_gate(places, n, dz), ready + [m for r in places for m in came_tok[r, dz]], 10))
    ups = ["G03", "G13", "G23"]
    for dz in REL:
        for dy in REL:
            for i in (0, 1):
                ready = have_uo(dz, dy) + have_up(dz, dy) + ["G10", "G20" if i else "G00"]
                ready = ready + [m for r in (2 * i, 2 * i + 1) for m in came_tok[r, dz]]
                ups.append("U%d%d%d" % (dz, dy, i))
                tasks.append(Task(ups[-1], 0.45, run_up(dz, dy, i), ready, 20 + i))
    tasks.append(Task("H", 0.5, run_hidden, ups, 0))
    blocks = sorted(((dz, dy) for dz in range(4) for dy in range(4)), key=lambda p: (min(p[0], 4 - p[0]) + min(p[1], 4 - p[1]), p))
    size = 128 * 256 * 2

    slot = {}

    def run_down(b, dz, dy):
        def run():
            j = plane(dz, dy)
            right = jnp.concatenate([db[j, 0], db[j, 1]], axis=1)

            def step(i, carry):
                left = hid[pl.ds(i * 2, 2)].reshape(512, 896)
                part = jnp.dot(left, right, preferred_element_type=F32).astype(BF).reshape(2, 2, 128, 256)
                summed[b, pl.ds(i * 2, 2)] = part[:, 0]
                psib[slot[b], pl.ds(i * 2, 2)] = part[:, 1]
                return carry

            lax.fori_loop(0, 2, step, 0)
        return run

    def run_add(b):
        def run():
            summed[b] = (summed[b].astype(F32) + rsib[b].astype(F32)).astype(BF)
        return run

    def run_merge(b):
        def run():
            if b % 2 == 0:
                summed[b, 1] = (summed[b, 1].astype(F32) + rl[b // 2].astype(F32)).astype(BF)
            else:
                summed[b, 3] = (summed[b, 3].astype(F32) + rr[b // 2].astype(F32)).astype(BF)
        return run

    def run_final(b, dz, dy):
        def run():
            total = summed[b, 0].astype(F32) + fl[b].astype(F32) + fr[b].astype(F32)
            columns = pl.ds(pl.multiple_of(plane(dz, dy) * 256, 256), 256)
            delta = jnp.dot(scaled[...], fup[:, columns], preferred_element_type=F32)
            base[:, columns] = (total + delta).astype(BF)
        return run

    hidden = ["H"]
    for b, (dz, dy) in enumerate(blocks):
        n, half = str(b), b // 2
        tasks.append(Task("D" + n, 1.25, run_down(b, dz, dy), hidden + have_do(dz, dy) + have_dp(dz, dy), 300 + b))
        add("Q" + n, "pair", 4 * size, None, rsib.at[b], rsib.at[b], ["D" + n])
        tasks.append(Task("A" + n, 0.15, run_add(b), ["D" + n, "Q" + n], 200 + b))
        if b % 2 == 0:
            add("Z" + n, "x+", size, summed.at[b, 2], rl.at[half], rl.at[half], ["A" + n], 10 + 3 * b)
            add("N" + n, "x-", size, summed.at[b, 3], fr.at[b], fr.at[b], ["A" + n], 12 + 3 * b)
            add("M" + n, "x+", size, summed.at[b, 1], fl.at[b], fl.at[b], ["C" + n], 11 + 3 * b)
        else:
            add("Z" + n, "x-", size, summed.at[b, 2], rr.at[half], rr.at[half], ["A" + n], 10 + 3 * b)
            add("N" + n, "x+", size, summed.at[b, 1], fl.at[b], fl.at[b], ["A" + n], 12 + 3 * b)
            add("M" + n, "x-", size, summed.at[b, 3], fr.at[b], fr.at[b], ["C" + n], 11 + 3 * b)
        tasks.append(Task("C" + n, 0.05, run_merge(b), ["A" + n, "Z" + n], 100 + b))
        tasks.append(Task("E" + n, 0.2, run_final(b, dz, dy), ["A" + n, "M" + n, "N" + n, "W0"], 400 + b))

    wide = 1152 * 4

    def run_low():
        mine = tok[0, 0]
        across = (((1,), (1,)), ((), ()))
        logits = lax.dot_general(mine, router[...], across, preferred_element_type=F32)
        first, second = small[:, 0:1], small[:, 1:2]
        expert = lax.broadcasted_iota(jnp.int32, (128, 8), 1)
        first_logit = jnp.sum(jnp.where(expert == first, logits, 0.0), axis=1, keepdims=True)
        second_logit = jnp.sum(jnp.where(expert == second, logits, 0.0), axis=1, keepdims=True)
        weight = jax.nn.sigmoid(first_logit - second_logit)
        column = lax.broadcasted_iota(jnp.int32, (128, 128), 1) // 16
        wide_coef = jnp.where(column == first, weight, jnp.where(column == second, 1.0 - weight, 0.0))
        coef[...] = wide_coef
        low = jnp.dot(mine, fdown[...], preferred_element_type=F32)
        value = (low * wide_coef).astype(BF)
        scaled[...] = value
        turned[1] = value.astype(F32).T.astype(BF)

    def run_dlow():
        cot[...] = cot[...] * small[:, 2:3].astype(F32).astype(BF)
        low = lax.dot_general(cot[...], fup[...], (((1,), (1,)), ((), ())), preferred_element_type=F32)
        turned[0] = (low * coef[...]).astype(BF).astype(F32).T.astype(BF)

    def local_part(owner, ab, h):
        columns = pl.ds(pl.multiple_of(owner * 2048 + ab * 1024, 1024), 1024)
        right = cot[:, columns] if h else tok[0, 0, :, columns]
        return jnp.dot(turned[h], right, preferred_element_type=F32)

    def count():
        return jnp.broadcast_to(jnp.sum(small[:, 2:3].astype(F32), axis=0, keepdims=True), (128, 128))

    tasks.append(Task("W0", 3.5, run_low, ["L", "LC"], 3))
    tasks.append(Task("W1", 2.5, run_dlow, ["W0"], 3))
    pieces = [(ab, h) for ab in range(2) for h in range(2)]
    for n, (ab, h) in enumerate(pieces):
        name = "PG%d%d" % (ab, h)

        def run_theirs(n=n, ab=ab, h=h):
            if n >= 2:
                early = by_name["PG%d%d" % pieces[n - 2]]
                descriptor(early, early.landing).wait_send()
            stage[n % 2, :, 0:1024] = local_part(1 - core, ab, h)
            stage[n % 2, :, 1024:1152] = count()

        def run_ours(ab=ab, h=h):
            rows = slice(h * 128, h * 128 + 128)
            g[ab, rows, 0:1024] += local_part(core, ab, h)
            g[ab, rows, 1024:1152] += count()

        landing = g.at[ab, pl.ds(h * 128, 128)]
        tasks.append(Task("WS%d%d" % (ab, h), 0.5, run_theirs, ["W1"] + (["WS%d%d" % pieces[n - 1]] if n else []), 3))
        add(name, "pair", 128 * wide, stage.at[n % 2], landing, landing, ["WS%d%d" % (ab, h)], 1)
        tasks.append(Task("WO%d%d" % (ab, h), 0.5, run_ours, [name, "W1"], 4))

    def reduce_ring(tag, axis, piece_at, hold_z, hold_m, rows, after, finish, rank):
        amount = rows * wide
        for sign, near, half in (("+", 1, 0), ("-", 3, 1)):
            add(tag + "Z" + sign, axis + sign, amount // 2, piece_at(2, half), hold_z.at[half], hold_z.at[half], after, rank)

            def combine(near=near, half=half):
                ref = piece_at(near, half)
                ref[...] = ref[...] + hold_z[half]

            tasks.append(Task(tag + "C" + sign, 0.2, combine, after + [tag + "Z" + sign], 6))
            add(tag + "M" + sign, axis + sign, amount, piece_at(near), hold_m.at[half], hold_m.at[half], [tag + "C" + sign], rank)
        tasks.append(Task(tag + "E", 0.3, finish, after + [tag + "M+", tag + "M-"], 6))

    row_of = {"y": y, "z": z}
    for ab, (first, second) in enumerate((("y", "z"), ("z", "y"))):
        p, q = row_of[first], row_of[second]

        def block(d, half=None, ab=ab, p=p):
            rows = pl.multiple_of(((p + d) % 4) * 64 + (half or 0) * 32, 32)
            return g.at[ab, pl.ds(rows, 64 if half is None else 32)]

        def slim(d, half=None, ab=ab, p=p, q=q):
            rows = pl.multiple_of(p * 64 + ((q + d) % 4) * 16 + (half or 0) * 8, 8)
            return g.at[ab, pl.ds(rows, 16 if half is None else 8)]

        z1, m1 = rz.at[ab, :, pl.ds(0, 32)], rm.at[ab, :, pl.ds(0, 64)]
        z2, m2 = rz.at[ab, :, pl.ds(32, 8)], rm.at[ab, :, pl.ds(64, 16)]

        def first_done(block=block, ab=ab):
            ref = block(0)
            ref[...] = ref[...] + rm[ab, 0, 0:64] + rm[ab, 1, 0:64]

        def second_done(slim=slim, ab=ab):
            xs[0, ab] = slim(0)[...] + rm[ab, 0, 64:80] + rm[ab, 1, 64:80]

        reduce_ring("R%d" % ab, first, block, z1, m1, 64, ["WO%d0" % ab, "WO%d1" % ab], first_done, GRAD_RANK)
        reduce_ring("S%d" % ab, second, slim, z2, m2, 16, ["R%dE" % ab], second_done, GRAD_RANK)

    slices = ["S0E", "S1E"]
    add("X+", "x+", 32 * wide, xs.at[0], xs.at[3], xs.at[3], slices, 6)
    add("X-", "x-", 32 * wide, xs.at[0], xs.at[1], xs.at[1], slices, 6)
    add("XF+", "x+", 16 * wide, xs.at[3, 0], xs.at[2, 0], xs.at[2, 0], ["X+"], 6)
    add("XF-", "x-", 16 * wide, xs.at[1, 1], xs.at[2, 1], xs.at[2, 1], ["X-"], 6)

    def row_block(ab, dz, dy):
        at_z, at_y = (z + dz) % 4, (y + dy) % 4
        return at_z * 4 + at_y if ab else at_y * 4 + at_z

    def run_whole():
        for ab in range(2):
            total = (xs[0, ab] + xs[2, ab]) + (xs[1, ab] + xs[3, ab])
            inverse = 1.0 / jnp.maximum(total[:, 1024:1025], 1.0)
            ga[ab, row_block(ab, 0, 0)] = (total[:, 0:1024] * inverse).astype(BF)

    tasks.append(Task("XS", 0.4, run_whole, slices + ["X+", "X-", "XF+", "XF-"], 6))
    for ab, first in enumerate("yz"):
        def finished(dz, dy, half, ab=ab):
            ref = ga.at[ab, row_block(ab, dz, dy)]
            return ref if half is None else ref.at[:, pl.ds(half * 512, 512)]

        have = spread("g%d" % ab, finished, 16 * 1024 * 2, first, ["XS"], GRAD_RANK)
        whole = sorted({n for dz in range(4) for dy in range(4) for n in have(dz, dy)})
        add("PH%d" % ab, "pair", 256 * 1024 * 2, ga.at[ab], gb.at[ab], gb.at[ab], whole)

    order, _ = arrange(copies, tasks, ["L", "LG", "LC"])
    assert len(copies) == COPIES
    place = {copy.name: i for i, copy in enumerate(copies)}
    by_name = {copy.name: copy for copy in copies}

    def descriptor(copy, landing):
        i = place[copy.name]
        return pltpu.make_async_remote_copy(
            src_ref=copy.source, dst_ref=landing, send_sem=send_sem.at[i], recv_sem=recv_sem.at[i],
            device_id=targets[copy.link], device_id_type=MESH)

    loads = [
        pltpu.make_async_copy(tokens, tok.at[0, 0], load_sem.at[0]),
        pltpu.make_async_copy(up.at[:, pl.ds(pl.multiple_of(xh * 896, 128), 896)], ub.at[plane(0, 0), xh], load_sem.at[1]),
        pltpu.make_async_copy(down.at[pl.ds(pl.multiple_of(xh * 896, 128), 896), :], db.at[plane(0, 0), xh], load_sem.at[2]),
    ]
    load_gate = pltpu.make_async_copy(gate.at[:, pl.ds(pl.multiple_of(xh * 896, 128), 896)], gw, load_sem.at[3])
    extra = [
        pltpu.make_async_copy(cotangent, cot, load_sem.at[4]),
        pltpu.make_async_copy(factors_down, fdown, load_sem.at[5]),
        pltpu.make_async_copy(factors_up, fup, load_sem.at[6]),
    ]
    for load in loads:
        load.start()
    for load in extra:
        load.start()
    load_gate.start()
    barrier = pltpu.get_barrier_semaphore()
    for target in targets.values():
        pl.semaphore_signal(barrier, inc=1, device_id=target, device_id_type=MESH)
    pl.semaphore_wait(barrier, len(targets))
    for load in loads:
        load.wait()
    gate_waited = False
    used = []
    for what, item in order:
        if item.name[0] == "D" and what == "task":
            if len(used) >= SLOTS:
                early = by_name["Q" + used[-SLOTS]]
                descriptor(early, early.landing).wait_send()
            slot[int(item.name[1:])] = len(used) % SLOTS
            used.append(item.name[1:])
            by_name["Q" + used[-1]].source = psib.at[slot[int(used[-1])]]
        if what == "send":
            descriptor(item, item.landing).start()
        elif what == "recv":
            descriptor(item, item.here).wait_recv()
        else:
            if item.name[0] == "G" and not gate_waited:
                load_gate.wait()
                gate_waited = True
            if item.name == "W0":
                for load in extra:
                    load.wait()
            item.run()
    stores = []
    for n, (half, whole) in enumerate(((core, ga), (1 - core, gb))):
        for ab in range(2):
            columns = pl.ds(pl.multiple_of(half * 2048 + ab * 1024, 1024), 1024)
            stores.append(pltpu.make_async_copy(whole.at[ab], grads.at[:, :, columns], load_sem.at[2 * n + ab]))
    for store in stores:
        store.start()
    already = {"Q" + n for n in used[:-SLOTS]} | {"PG00", "PG01"}
    for copy in copies:
        if copy.name not in already:
            descriptor(copy, copy.landing).wait_send()
    for store in stores:
        store.wait()


COPIES = 8 + 28 + 64 + 64 + 4 + 16 + 4 + 32 + 2


def layer(*operands):
    hbm = pl.BlockSpec(memory_space=pl.ANY)
    return pl.pallas_call(
        kernel,
        out_shape=(jax.ShapeDtypeStruct((128, 4096), BF), jax.ShapeDtypeStruct((16, 16, 4096), BF)),
        in_specs=[hbm] * 7 + [pl.BlockSpec(memory_space=pltpu.VMEM)] * 2,
        out_specs=(pl.BlockSpec(memory_space=pltpu.VMEM), hbm),
        scratch_shapes=[
            pltpu.VMEM((4, 2, 128, 4096), BF),
            pltpu.VMEM((4096, 896), BF),
            pltpu.VMEM((16, 2, 128, 896), BF),
            pltpu.VMEM((16, 2, 896, 128), BF),
            pltpu.VMEM((4, 256, 896), F32),
            pltpu.VMEM((4, 256, 896), F32),
            pltpu.VMEM((4, 256, 896), BF),
            pltpu.VMEM((SLOTS, 4, 128, 256), BF),
            pltpu.VMEM((16, 4, 128, 256), BF),
            pltpu.VMEM((16, 4, 128, 256), BF),
            pltpu.VMEM((8, 128, 256), BF),
            pltpu.VMEM((8, 128, 256), BF),
            pltpu.VMEM((16, 128, 256), BF),
            pltpu.VMEM((16, 128, 256), BF),
            pltpu.VMEM((2, 64, 896), BF),
            pltpu.VMEM((2, 448, 128), BF),
            pltpu.VMEM((2, 256, 1152), F32),
            pltpu.VMEM((2, 128, 1152), F32),
            pltpu.VMEM((128, 4096), BF),
            pltpu.VMEM((4096, 128), BF),
            pltpu.VMEM((128, 4096), BF),
            pltpu.VMEM((128, 128), F32),
            pltpu.VMEM((128, 128), BF),
            pltpu.VMEM((2, 128, 128), BF),
            pltpu.VMEM((2, 2, 40, 1152), F32),
            pltpu.VMEM((2, 2, 80, 1152), F32),
            pltpu.VMEM((4, 2, 16, 1152), F32),
            pltpu.VMEM((2, 16, 16, 1024), BF),
            pltpu.VMEM((2, 16, 16, 1024), BF),
            pltpu.SemaphoreType.DMA((7,)),
            pltpu.SemaphoreType.DMA((COPIES,)),
            pltpu.SemaphoreType.DMA((COPIES,)),
        ],
        compiler_params=pltpu.CompilerParams(
            collective_id=0, has_side_effects=True, vmem_limit_bytes=67_000_000),
        cost_estimate=pl.CostEstimate(flops=22_500_000_000, bytes_accessed=16_000_000, transcendentals=1_000_000),
        name="layer",
    )(*operands)


def shards(
    tokens,
    gate_projection_weight,
    up_projection_weight,
    down_projection_weight,
    router_projection_weight,
    adapter_down_factors,
    adapter_up_factors,
    routes,
    padding_token_mask,
    cotangent,
):
    small = jnp.concatenate([routes, padding_token_mask[:, None]], axis=1)
    layer_out, grads = layer(
        tokens, gate_projection_weight, up_projection_weight, down_projection_weight,
        cotangent, adapter_down_factors, adapter_up_factors, router_projection_weight.T, small)
    rows = grads.reshape(256, 4096)
    grad_down = rows[:128].astype(F32).T
    grad_up = rows[128:].astype(F32)
    return (layer_out, grad_down, grad_up)


def solution(mesh):
    return jax.shard_map(
        shards,
        mesh=mesh,
        in_specs=(
            P(("dp", "blk"), None),
            P(None, "blk"),
            P("dp", "blk"),
            P("blk", "dp"),
            P(),
            P(),
            P(),
            P(("dp", "blk"), None),
            P(("dp", "blk")),
            P(("dp", "blk"), None),
        ),
        out_specs=(P(("dp", "blk"), None), P(), P()),
        check_vma=False,
    )
```

```python
import jax
import jax.numpy as jnp
from jax import lax
from jax.experimental import pallas as pl
from jax.experimental.pallas import tpu as pltpu
from jax.sharding import PartitionSpec as P

MESH = pl.DeviceIdType.MESH
BF, F32 = jnp.bfloat16, jnp.float32

REL = (0, 1, 3, 2)
LINK_RATE, PAIR_RATE = 46.6e3, 300e3
HOP, PAIR_HOP = 1.8, 1.0
AHEAD = 2.5
GRAD_RANK = 50
SLOTS = 3


COPY_RANKS = (
    -1035, -564, -297, -1186, 1297, -323, 83, -1833, 1126, 2034, 74, 1002, -117, -115, -1310, 2730, -2076, -686, 1585, 164, 950, -354, 945, 1560,
    -262, 1893, 573, -2310, -928, 441, -1189, -117, -688, 2744, 995, 3082, 29, 1463, 411, -1001, -1815, 1111, 167, -1630, -161, -105, 1228, 805,
    337, -717, -300, 1439, -1755, -1329, 1111, -245, -427, -477, -193, 397, 409, 915, 1009, -310, -571, -1651, -684, -542, 459, -1420, 227, -1145,
    290, 2251, 1456, -337, 2771, 2945, 3560, 2121, 232, -953, -1179, 495, 1369, 110, -1722, -1659, 1144, 630, 2707, -270, -1954, 461, 703, -999,
    -562, -908, 1400, 1249, 534, -173, -2003, -144, -787, 363, -21, -1398, 1473, 27, 714, 433, -741, 470, 1795, -1568, 727, -969, -721, -177,
    -1276, -13, 2564, 3224, 39, 620, 1402, -962, -1736, 715, 785, 1952, 934, -1287, -1151, 1553, 807, -1691, 209, 2356, 466, -1055, 533, -106,
    931, 2818, -2301, 1912, 2921, -956, 195, 1857, 2449, 1351, 683, 623, 620, 1382, -1203, 580, -344, 58, 328, 63, 1143, 498, -1147, 13,
    810, 1313, 256, -132, -421, -674, 946, 1349, 226, 1417, 209, 320, 314, 43, 917, -362, 1870, -1583, -1719, -301, 615, -1421, -106, 655,
    652, -898, -451, 85, -650, 855, 1004, 800, 273, -2679, 553, 1105, 1057, -175, 284, -1020, -118, 1689, 1643, -206, 1655, 322, -1652, 325,
    -334, 1821, -332, -622, 1228, 2296,
)
TASK_RANKS = (
    -33, -1131, 1174, 1480, 1485, -2499, 257, -1955, -430, 1137, 287, 345, -2437, -385, 2439, 2912, -415, -1261, 1884, -1054, 293, 2581, -656, -5095,
    -347, 524, -2374, 2182, 455, 1020, -366, -2587, -2489, -622, -2566, -321, -3481, -4440, -106, -5293, 1667, -2396, 591, 294, -1230, 1401, -721, 171,
    1110, 385, -1132, -2307, -715, 1876, 2225, -1705, -2537, 662, 699, 2304, 192, 905, 475, 828, -1543, 2065, 417, 2995, 1855, -1717, -2158, -210,
    3577, 2676, -837, 944, 1596, 2779, -2082, -811, 414, 398, -425, 778, -633, 1703, 792, -1676, -656, 1519, 1951, 206, 1324, 1066, -56, -2582,
    -239, 2270, -2355, 2041, -637, 606, 1027, 1011, 158, 2195, 194, 2230, -4962, 2123, 476, 170, 2020, 1369, -1719, -1455, 2186, 850, -1015, 506,
    997, -1799, 754, -543, 1685, -2714, -393, -975, -237, 74, 1887, 2352,
)


class Copy:
    def __init__(self, name, link, size, source, landing, here, rank):
        self.name, self.link, self.size, self.rank = name, link, size, rank
        self.source, self.landing, self.here = source, landing, here
        self.after = set()


class Task:
    def __init__(self, name, cost, run, after, rank):
        self.name, self.cost, self.run, self.after, self.rank = name, cost, run, set(after), rank


def arrange(copies, tasks, begun):
    order, done, now = [], set(begun), 0.0
    free, arriving, queued = {}, [], {}
    to_send, to_run = list(copies), list(tasks)

    def send(copy):
        order.append(("send", copy))
        rate, hop = (PAIR_RATE, PAIR_HOP) if copy.link == "pair" else (LINK_RATE, HOP)
        start = max(now, free.get(copy.link, 0.0))
        free[copy.link] = end = start + copy.size / rate
        arriving.append((end + hop, copy))

    def send_ready(until):
        for copy in list(to_send):
            if copy.after <= done:
                to_send.remove(copy)
                queued.setdefault(copy.link, []).append(copy)
        for link, line in queued.items():
            line.sort(key=lambda copy: copy.rank)
            while line and (free.get(link, 0.0) < until or link == "pair"):
                send(line.pop(0))

    send_ready(AHEAD)
    while arriving or to_run:
        arriving.sort(key=lambda pair: pair[0])
        ready = [task for task in to_run if task.after <= done]
        if arriving and arriving[0][0] <= now:
            copy = arriving.pop(0)[1]
            order.append(("recv", copy))
            done.add(copy.name)
            send_ready(now + AHEAD)
        elif ready:
            task = min(ready, key=lambda task: task.rank)
            to_run.remove(task)
            order.append(("task", task))
            now += task.cost
            done.add(task.name)
            send_ready(now + AHEAD)
        else:
            send_ready(arriving[0][0] + AHEAD)
            arriving.sort(key=lambda pair: pair[0])
            now = arriving[0][0]
    assert not to_send
    return order, now


def kernel(tokens, gate, up, down, cotangent, factors_down, factors_up, router, small, base, grads_low, grads_high, tok, gw, ub, db, gact, uact, hid, psib, rsib, summed,
           rl, rr, fl, fr, ustage, dstage, g, stage, cot, fdown, fup, coef, scaled, turned, rz, rm, xs, ga, gb, load_sem, send_sem, recv_sem):
    dp, blk = lax.axis_index("dp"), lax.axis_index("blk")
    z, y, xh = dp // 8, (dp // 2) % 4, dp % 2
    xl, core = blk // 2, blk % 2
    x = xh * 2 + xl

    def device(dz=0, dy=0, dx=0, dc=0):
        at_z, at_y, at_x = (z + dz) % 4, (y + dy) % 4, (x + dx) % 4
        return ((at_z * 4 + at_y) * 2 + at_x // 2, (at_x % 2) * 2 + (core + dc) % 2)

    targets = {
        "z+": device(dz=1), "z-": device(dz=3), "y+": device(dy=1), "y-": device(dy=3),
        "x+": device(dx=1), "x-": device(dx=3), "pair": device(dc=1),
    }

    def plane(dz, dy):
        return ((z + dz) % 4) * 4 + (y + dy) % 4

    copies = []

    def add(name, link, size, source, landing, here, after=(), rank=0):
        copy = Copy(name, link, size, source, landing, here, rank)
        copy.after = set(after)
        copies.append(copy)
        return copy

    piece = 128 * 896 * 2

    def weight(kind, dz, dy, own, half=None):
        ref, rows = (ub, 128) if kind == "u" else (db, 896)
        ref = ref.at[plane(dz, dy), xh if own else 1 - xh]
        if half is None:
            return ref
        return ref.at[pl.ds(half * (rows // 2), rows // 2)]

    def spread(tag, ref, size, first, origin, base_rank):
        second = "z" if first == "y" else "y"

        def at(f, s, half=None):
            return ref(f, s, half) if first == "z" else ref(s, f, half)

        def move(name, link, f, s, f_new, s_new, after, rank, half=None):
            amount = size if half is None else size // 2
            add(tag + name, link, amount, at(f, s, half), at(f, s, half), at(f_new, s_new, half), after, rank + base_rank)

        move("F+", first + "+", 0, 0, 3, 0, origin, 0)
        move("F-", first + "-", 0, 0, 1, 0, origin, 0)
        move("S+0", second + "+", 0, 0, 0, 3, origin, 1)
        move("S-0", second + "-", 0, 0, 0, 1, origin, 1)
        move("G+", first + "+", 3, 0, 2, 0, [tag + "F+"], 2, 0)
        move("G-", first + "-", 1, 0, 2, 0, [tag + "F-"], 2, 1)
        came = {0: origin, 3: [tag + "F+"], 1: [tag + "F-"], 2: [tag + "G+", tag + "G-"]}
        for f in REL[1:]:
            move("S+%d" % f, second + "+", f, 0, f, 3, came[f], 4 if f == 2 else 3)
            move("S-%d" % f, second + "-", f, 0, f, 1, came[f], 4 if f == 2 else 3)
        for f in (0, 1):
            move("T+%d" % f, second + "+", f, 3, f, 2, [tag + "S+%d" % f], 5)
        for f in (3, 2):
            move("T-%d" % f, second + "-", f, 1, f, 2, [tag + "S-%d" % f], 5)

        def have(f, s):
            if s == 0:
                return came[f]
            if s == 3:
                return [tag + "S+%d" % f]
            if s == 1:
                return [tag + "S-%d" % f]
            return [tag + ("T+%d" if f in (0, 1) else "T-%d") % f]

        return (lambda dz, dy: have(dz, dy)) if first == "z" else (lambda dz, dy: have(dy, dz))

    def across(kind, hbm, ref, stage, rows, rank):
        for sign, step, half in (("+", 1, 0), ("-", 3, 1)):
            part = pl.ds(half * rows, rows)
            if kind == "u":
                source = hbm.at[part, pl.ds(pl.multiple_of((1 - xh) * 896, 128), 896)]
            else:
                source = hbm.at[pl.ds(pl.multiple_of((1 - xh) * 896 + half * rows, 64), rows), :]
            next_half = 1 - ((x + step) % 4) // 2
            hold = stage.at[half]
            add("A" + kind + sign, "x" + sign, piece // 2, source, hold, hold, [], rank)
            add("B" + kind + sign, "x" + sign, piece // 2, hold, ref.at[plane(0, 0), next_half, part],
                ref.at[plane(0, 0), 1 - xh, part], ["A" + kind + sign], rank)
        return ["B" + kind + "+", "B" + kind + "-"]

    mib = 128 * 4096 * 2
    have_au = across("u", up, ub, ustage, 64, 0)
    def columns_of(dz):
        return pl.ds(pl.multiple_of(((z + dz) % 4) * 1024, 1024), 1024)

    def some(r, c, dz):
        return tok.at[r, c, :, columns_of(dz)]

    came_tok = {}
    for dz in REL:
        came_tok[0, dz] = ["L"]
        for sign, r in (("+", 3), ("-", 1)):
            add("K%s%d" % (sign, dz), "x" + sign, mib // 4, some(0, 0, dz), some(r, 0, dz), some(r, 0, dz), ["L", "Au" + sign], 3)
            came_tok[r, dz] = ["K%s%d" % (sign, dz)]
        sign, r = ("+", 3) if dz < 2 else ("-", 1)
        add("KF%d" % dz, "x" + sign, mib // 4, some(r, 0, dz), some(2, 0, dz), some(2, 0, dz), came_tok[r, dz], 4)
        came_tok[2, dz] = ["KF%d" % dz]
        for r in REL:
            add("KS%d%d" % (r, dz), "pair", mib // 4, some(r, 0, dz), some(r, 1, dz), some(r, 1, dz), came_tok[r, dz])
            came_tok[r, dz] = came_tok[r, dz] + ["KS%d%d" % (r, dz)]
    have_ad = across("d", down, db, dstage, 448, 5)
    def piece_of(kind, own):
        return lambda dz, dy, half: weight(kind, dz, dy, own, half)

    have_uo = spread("uo", piece_of("u", True), piece, "y", ["L"], 0)
    have_up = spread("up", piece_of("u", False), piece, "z", have_au, 0)
    have_do = spread("do", piece_of("d", True), piece, "z", ["L"], 100)
    have_dp = spread("dp", piece_of("d", False), piece, "y", have_ad, 100)

    tasks = []

    def run_gate(places, n, dz):
        def run():
            def step(i, carry):
                k = pl.multiple_of(((z + dz) % 4) * 1024 + i * 512, 512)
                left = jnp.concatenate([tok[r, :, :, pl.ds(k, 512)].reshape(256, 512) for r in places], axis=0)
                part = jnp.dot(left, gw[pl.ds(k, 512), :], preferred_element_type=F32)
                for m, r in enumerate(places):
                    gact[r] += part[m * 256:m * 256 + 256]
                return carry

            if n == 0:
                for r in places:
                    gact[r] = jnp.zeros((256, 896), F32)
                    uact[r] = jnp.zeros((256, 896), F32)
            lax.fori_loop(0, 2, step, 0)
            if n == 3:
                for r in places:
                    v = gact[r]
                    gact[r] = v / (1.0 + jnp.exp(-v))
        return run

    def run_up(dz, dy, i):
        def run():
            j = plane(dz, dy)
            columns = pl.ds(pl.multiple_of(j * 256, 256), 256)
            two = pl.ds(i * 2, 2)
            left = tok[two, :, :, columns].reshape(512, 256)
            part = jnp.dot(left, ub[j].reshape(256, 896), preferred_element_type=F32)
            uact[two] += part.reshape(2, 256, 896)
        return run

    def run_hidden():
        hid[...] = (gact[...] * uact[...]).astype(BF)

    ups = []
    for name, cost, places in (("G0", 1.4, (0,)), ("G1", 2.2, (1, 3)), ("G2", 1.4, (2,))):
        for n, dz in enumerate(REL):
            ready = [name + str(n - 1)] if n else ["LG"]
            tasks.append(Task(name + str(n), cost, run_gate(places, n, dz), ready + [m for r in places for m in came_tok[r, dz]], 10))
    ups = ["G03", "G13", "G23"]
    for dz in REL:
        for dy in REL:
            for i in (0, 1):
                ready = have_uo(dz, dy) + have_up(dz, dy) + ["G10", "G20" if i else "G00"]
                ready = ready + [m for r in (2 * i, 2 * i + 1) for m in came_tok[r, dz]]
                ups.append("U%d%d%d" % (dz, dy, i))
                tasks.append(Task(ups[-1], 0.45, run_up(dz, dy, i), ready, 20 + i))
    tasks.append(Task("H", 0.5, run_hidden, ups, 0))
    blocks = sorted(((dz, dy) for dz in range(4) for dy in range(4)), key=lambda p: (min(p[0], 4 - p[0]) + min(p[1], 4 - p[1]), p))
    size = 128 * 256 * 2

    slot = {}

    def run_down(b, dz, dy):
        def run():
            j = plane(dz, dy)
            right = jnp.concatenate([db[j, 0], db[j, 1]], axis=1)

            def step(i, carry):
                left = hid[pl.ds(i * 2, 2)].reshape(512, 896)
                part = jnp.dot(left, right, preferred_element_type=F32).astype(BF).reshape(2, 2, 128, 256)
                summed[b, pl.ds(i * 2, 2)] = part[:, 0]
                psib[slot[b], pl.ds(i * 2, 2)] = part[:, 1]
                return carry

            lax.fori_loop(0, 2, step, 0)
        return run

    def run_add(b):
        def run():
            summed[b] = (summed[b].astype(F32) + rsib[b].astype(F32)).astype(BF)
        return run

    def run_merge(b):
        def run():
            if b % 2 == 0:
                summed[b, 1] = (summed[b, 1].astype(F32) + rl[b // 2].astype(F32)).astype(BF)
            else:
                summed[b, 3] = (summed[b, 3].astype(F32) + rr[b // 2].astype(F32)).astype(BF)
        return run

    def run_final(b, dz, dy):
        def run():
            total = summed[b, 0].astype(F32) + fl[b].astype(F32) + fr[b].astype(F32)
            columns = pl.ds(pl.multiple_of(plane(dz, dy) * 256, 256), 256)
            delta = jnp.dot(scaled[...], fup[:, columns], preferred_element_type=F32)
            base[:, columns] = (total + delta).astype(BF)
        return run

    hidden = ["H"]
    for b, (dz, dy) in enumerate(blocks):
        n, half = str(b), b // 2
        tasks.append(Task("D" + n, 1.25, run_down(b, dz, dy), hidden + have_do(dz, dy) + have_dp(dz, dy), 300 + b))
        add("Q" + n, "pair", 4 * size, None, rsib.at[b], rsib.at[b], ["D" + n])
        tasks.append(Task("A" + n, 0.15, run_add(b), ["D" + n, "Q" + n], 200 + b))
        if b % 2 == 0:
            add("Z" + n, "x+", size, summed.at[b, 2], rl.at[half], rl.at[half], ["A" + n], 10 + 3 * b)
            add("N" + n, "x-", size, summed.at[b, 3], fr.at[b], fr.at[b], ["A" + n], 12 + 3 * b)
            add("M" + n, "x+", size, summed.at[b, 1], fl.at[b], fl.at[b], ["C" + n], 11 + 3 * b)
        else:
            add("Z" + n, "x-", size, summed.at[b, 2], rr.at[half], rr.at[half], ["A" + n], 10 + 3 * b)
            add("N" + n, "x+", size, summed.at[b, 1], fl.at[b], fl.at[b], ["A" + n], 12 + 3 * b)
            add("M" + n, "x-", size, summed.at[b, 3], fr.at[b], fr.at[b], ["C" + n], 11 + 3 * b)
        tasks.append(Task("C" + n, 0.05, run_merge(b), ["A" + n, "Z" + n], 100 + b))
        tasks.append(Task("E" + n, 0.2, run_final(b, dz, dy), ["A" + n, "M" + n, "N" + n, "W0"], 400 + b))

    wide = 1152 * 4

    def run_low():
        mine = tok[0, 0]
        across = (((1,), (1,)), ((), ()))
        logits = lax.dot_general(mine, router[...], across, preferred_element_type=F32)
        first, second = small[:, 0:1], small[:, 1:2]
        expert = lax.broadcasted_iota(jnp.int32, (128, 8), 1)
        first_logit = jnp.sum(jnp.where(expert == first, logits, 0.0), axis=1, keepdims=True)
        second_logit = jnp.sum(jnp.where(expert == second, logits, 0.0), axis=1, keepdims=True)
        weight = jax.nn.sigmoid(first_logit - second_logit)
        column = lax.broadcasted_iota(jnp.int32, (128, 128), 1) // 16
        wide_coef = jnp.where(column == first, weight, jnp.where(column == second, 1.0 - weight, 0.0))
        coef[...] = wide_coef
        low = jnp.dot(mine, fdown[...], preferred_element_type=F32)
        value = (low * wide_coef).astype(BF)
        scaled[...] = value
        turned[1] = value.astype(F32).T.astype(BF)

    def run_dlow():
        cot[...] = cot[...] * small[:, 2:3].astype(F32).astype(BF)
        low = lax.dot_general(cot[...], fup[...], (((1,), (1,)), ((), ())), preferred_element_type=F32)
        turned[0] = (low * coef[...]).astype(BF).astype(F32).T.astype(BF)

    def local_part(owner, ab, h):
        columns = pl.ds(pl.multiple_of(owner * 2048 + ab * 1024, 1024), 1024)
        right = cot[:, columns] if h else tok[0, 0, :, columns]
        return jnp.dot(turned[h], right, preferred_element_type=F32)

    def count():
        return jnp.broadcast_to(jnp.sum(small[:, 2:3].astype(F32), axis=0, keepdims=True), (128, 128))

    tasks.append(Task("W0", 3.5, run_low, ["L", "LC"], 3))
    tasks.append(Task("W1", 2.5, run_dlow, ["W0"], 3))
    pieces = [(ab, h) for ab in range(2) for h in range(2)]
    for n, (ab, h) in enumerate(pieces):
        name = "PG%d%d" % (ab, h)

        def run_theirs(n=n, ab=ab, h=h):
            if n >= 2:
                early = by_name["PG%d%d" % pieces[n - 2]]
                descriptor(early, early.landing).wait_send()
            stage[n % 2, :, 0:1024] = local_part(1 - core, ab, h)
            stage[n % 2, :, 1024:1152] = count()

        def run_ours(ab=ab, h=h):
            rows = slice(h * 128, h * 128 + 128)
            g[ab, rows, 0:1024] += local_part(core, ab, h)
            g[ab, rows, 1024:1152] += count()

        landing = g.at[ab, pl.ds(h * 128, 128)]
        tasks.append(Task("WS%d%d" % (ab, h), 0.5, run_theirs, ["W1"] + (["WS%d%d" % pieces[n - 1]] if n else []), 3))
        add(name, "pair", 128 * wide, stage.at[n % 2], landing, landing, ["WS%d%d" % (ab, h)], 1)
        tasks.append(Task("WO%d%d" % (ab, h), 0.5, run_ours, [name, "W1"], 4))

    def reduce_ring(tag, axis, piece_at, hold_z, hold_m, rows, after, finish, rank):
        amount = rows * wide
        for sign, near, half in (("+", 1, 0), ("-", 3, 1)):
            add(tag + "Z" + sign, axis + sign, amount // 2, piece_at(2, half), hold_z.at[half], hold_z.at[half], after, rank)

            def combine(near=near, half=half):
                ref = piece_at(near, half)
                ref[...] = ref[...] + hold_z[half]

            tasks.append(Task(tag + "C" + sign, 0.2, combine, after + [tag + "Z" + sign], 6))
            add(tag + "M" + sign, axis + sign, amount, piece_at(near), hold_m.at[half], hold_m.at[half], [tag + "C" + sign], rank)
        tasks.append(Task(tag + "E", 0.3, finish, after + [tag + "M+", tag + "M-"], 6))

    row_of = {"y": y, "z": z}
    for ab, (first, second) in enumerate((("y", "z"), ("z", "y"))):
        p, q = row_of[first], row_of[second]

        def block(d, half=None, ab=ab, p=p):
            rows = pl.multiple_of(((p + d) % 4) * 64 + (half or 0) * 32, 32)
            return g.at[ab, pl.ds(rows, 64 if half is None else 32)]

        def slim(d, half=None, ab=ab, p=p, q=q):
            rows = pl.multiple_of(p * 64 + ((q + d) % 4) * 16 + (half or 0) * 8, 8)
            return g.at[ab, pl.ds(rows, 16 if half is None else 8)]

        z1, m1 = rz.at[ab, :, pl.ds(0, 32)], rm.at[ab, :, pl.ds(0, 64)]
        z2, m2 = rz.at[ab, :, pl.ds(32, 8)], rm.at[ab, :, pl.ds(64, 16)]

        def first_done(block=block, ab=ab):
            ref = block(0)
            ref[...] = ref[...] + rm[ab, 0, 0:64] + rm[ab, 1, 0:64]

        def second_done(slim=slim, ab=ab):
            xs[0, ab] = slim(0)[...] + rm[ab, 0, 64:80] + rm[ab, 1, 64:80]

        reduce_ring("R%d" % ab, first, block, z1, m1, 64, ["WO%d0" % ab, "WO%d1" % ab], first_done, GRAD_RANK)
        reduce_ring("S%d" % ab, second, slim, z2, m2, 16, ["R%dE" % ab], second_done, GRAD_RANK)

    slices = ["S0E", "S1E"]
    add("X+", "x+", 32 * wide, xs.at[0], xs.at[3], xs.at[3], slices, 6)
    add("X-", "x-", 32 * wide, xs.at[0], xs.at[1], xs.at[1], slices, 6)
    add("XF+", "x+", 16 * wide, xs.at[3, 0], xs.at[2, 0], xs.at[2, 0], ["X+"], 6)
    add("XF-", "x-", 16 * wide, xs.at[1, 1], xs.at[2, 1], xs.at[2, 1], ["X-"], 6)

    def row_block(ab, dz, dy):
        at_z, at_y = (z + dz) % 4, (y + dy) % 4
        return at_z * 4 + at_y if ab else at_y * 4 + at_z

    def run_whole():
        for ab in range(2):
            total = (xs[0, ab] + xs[2, ab]) + (xs[1, ab] + xs[3, ab])
            inverse = 1.0 / jnp.maximum(total[:, 1024:1025], 1.0)
            ga[ab, row_block(ab, 0, 0)] = (total[:, 0:1024] * inverse).astype(BF)

    tasks.append(Task("XS", 0.4, run_whole, slices + ["X+", "X-", "XF+", "XF-"], 6))
    for ab, first in enumerate("yz"):
        def finished(dz, dy, half, ab=ab):
            ref = ga.at[ab, row_block(ab, dz, dy)]
            return ref if half is None else ref.at[:, pl.ds(half * 512, 512)]

        have = spread("g%d" % ab, finished, 16 * 1024 * 2, first, ["XS"], GRAD_RANK)
        whole = sorted({n for dz in range(4) for dy in range(4) for n in have(dz, dy)})
        add("PH%d" % ab, "pair", 256 * 1024 * 2, ga.at[ab], gb.at[ab], gb.at[ab], whole)

    for item, rank in zip(copies + tasks, COPY_RANKS + TASK_RANKS, strict=True):
        item.rank = rank
    for item, rank in zip(copies + tasks, COPY_RANKS + TASK_RANKS, strict=True):
        item.rank = rank
    order, _ = arrange(copies, tasks, ["L", "LG", "LC"])
    assert len(copies) == COPIES
    place = {copy.name: i for i, copy in enumerate(copies)}
    by_name = {copy.name: copy for copy in copies}

    def descriptor(copy, landing):
        i = place[copy.name]
        return pltpu.make_async_remote_copy(
            src_ref=copy.source, dst_ref=landing, send_sem=send_sem.at[i], recv_sem=recv_sem.at[i],
            device_id=targets[copy.link], device_id_type=MESH)

    loads = [
        pltpu.make_async_copy(tokens, tok.at[0, 0], load_sem.at[0]),
        pltpu.make_async_copy(up.at[:, pl.ds(pl.multiple_of(xh * 896, 128), 896)], ub.at[plane(0, 0), xh], load_sem.at[1]),
        pltpu.make_async_copy(down.at[pl.ds(pl.multiple_of(xh * 896, 128), 896), :], db.at[plane(0, 0), xh], load_sem.at[2]),
    ]
    load_gate = pltpu.make_async_copy(gate.at[:, pl.ds(pl.multiple_of(xh * 896, 128), 896)], gw, load_sem.at[3])
    extra = [
        pltpu.make_async_copy(cotangent, cot, load_sem.at[4]),
        pltpu.make_async_copy(factors_down, fdown, load_sem.at[5]),
        pltpu.make_async_copy(factors_up, fup, load_sem.at[6]),
    ]
    for load in loads:
        load.start()
    for load in extra:
        load.start()
    load_gate.start()
    barrier = pltpu.get_barrier_semaphore()
    for target in targets.values():
        pl.semaphore_signal(barrier, inc=1, device_id=target, device_id_type=MESH)
    pl.semaphore_wait(barrier, len(targets))
    for load in loads:
        load.wait()
    gate_waited = False
    used = []
    for what, item in order:
        if item.name[0] == "D" and what == "task":
            if len(used) >= SLOTS:
                early = by_name["Q" + used[-SLOTS]]
                descriptor(early, early.landing).wait_send()
            slot[int(item.name[1:])] = len(used) % SLOTS
            used.append(item.name[1:])
            by_name["Q" + used[-1]].source = psib.at[slot[int(used[-1])]]
        if what == "send":
            descriptor(item, item.landing).start()
        elif what == "recv":
            descriptor(item, item.here).wait_recv()
        else:
            if item.name[0] == "G" and not gate_waited:
                load_gate.wait()
                gate_waited = True
            if item.name == "W0":
                for load in extra:
                    load.wait()
            item.run()
    stores = []
    for half, whole in ((core, ga), (1 - core, gb)):
        for ab in range(2):
            columns = pl.ds(pl.multiple_of(half * 2048 + ab * 1024, 1024), 1024)
            for n, result in enumerate((grads_low, grads_high)):
                part = whole.at[ab, pl.ds(8 * n, 8)]
                stores.append(pltpu.make_async_copy(part, result.at[:, :, columns], load_sem.at[len(stores)]))
    for store in stores:
        store.start()
    already = {"Q" + n for n in used[:-SLOTS]} | {"PG00", "PG01"}
    for copy in copies:
        if copy.name not in already:
            descriptor(copy, copy.landing).wait_send()
    for store in stores:
        store.wait()


COPIES = 8 + 28 + 64 + 64 + 4 + 16 + 4 + 32 + 2


def layer(*operands):
    hbm = pl.BlockSpec(memory_space=pl.ANY)
    return pl.pallas_call(
        kernel,
        out_shape=(jax.ShapeDtypeStruct((128, 4096), BF), jax.ShapeDtypeStruct((8, 16, 4096), BF), jax.ShapeDtypeStruct((8, 16, 4096), BF)),
        in_specs=[hbm] * 7 + [pl.BlockSpec(memory_space=pltpu.VMEM)] * 2,
        out_specs=(pl.BlockSpec(memory_space=pltpu.VMEM), hbm, hbm),
        scratch_shapes=[
            pltpu.VMEM((4, 2, 128, 4096), BF),
            pltpu.VMEM((4096, 896), BF),
            pltpu.VMEM((16, 2, 128, 896), BF),
            pltpu.VMEM((16, 2, 896, 128), BF),
            pltpu.VMEM((4, 256, 896), F32),
            pltpu.VMEM((4, 256, 896), F32),
            pltpu.VMEM((4, 256, 896), BF),
            pltpu.VMEM((SLOTS, 4, 128, 256), BF),
            pltpu.VMEM((16, 4, 128, 256), BF),
            pltpu.VMEM((16, 4, 128, 256), BF),
            pltpu.VMEM((8, 128, 256), BF),
            pltpu.VMEM((8, 128, 256), BF),
            pltpu.VMEM((16, 128, 256), BF),
            pltpu.VMEM((16, 128, 256), BF),
            pltpu.VMEM((2, 64, 896), BF),
            pltpu.VMEM((2, 448, 128), BF),
            pltpu.VMEM((2, 256, 1152), F32),
            pltpu.VMEM((2, 128, 1152), F32),
            pltpu.VMEM((128, 4096), BF),
            pltpu.VMEM((4096, 128), BF),
            pltpu.VMEM((128, 4096), BF),
            pltpu.VMEM((128, 128), F32),
            pltpu.VMEM((128, 128), BF),
            pltpu.VMEM((2, 128, 128), BF),
            pltpu.VMEM((2, 2, 40, 1152), F32),
            pltpu.VMEM((2, 2, 80, 1152), F32),
            pltpu.VMEM((4, 2, 16, 1152), F32),
            pltpu.VMEM((2, 16, 16, 1024), BF),
            pltpu.VMEM((2, 16, 16, 1024), BF),
            pltpu.SemaphoreType.DMA((8,)),
            pltpu.SemaphoreType.DMA((COPIES,)),
            pltpu.SemaphoreType.DMA((COPIES,)),
        ],
        compiler_params=pltpu.CompilerParams(
            collective_id=0, has_side_effects=True, vmem_limit_bytes=67_000_000),
        cost_estimate=pl.CostEstimate(flops=22_500_000_000, bytes_accessed=16_000_000, transcendentals=1_000_000),
        name="layer",
    )(*operands)


def shards(
    tokens,
    gate_projection_weight,
    up_projection_weight,
    down_projection_weight,
    router_projection_weight,
    adapter_down_factors,
    adapter_up_factors,
    routes,
    padding_token_mask,
    cotangent,
):
    small = jnp.concatenate([routes, padding_token_mask[:, None]], axis=1)
    layer_out, grads_low, grads_high = layer(
        tokens, gate_projection_weight, up_projection_weight, down_projection_weight,
        cotangent, adapter_down_factors, adapter_up_factors, router_projection_weight.T, small)
    unit = jnp.eye(128, dtype=BF)
    grad_down = lax.dot_general(grads_low.reshape(128, 4096), unit, (((0,), (0,)), ((), ())), preferred_element_type=F32)
    grad_up = grads_high.reshape(128, 4096).astype(F32)
    return (layer_out, grad_down, grad_up)


def solution(mesh):
    return jax.shard_map(
        shards,
        mesh=mesh,
        in_specs=(
            P(("dp", "blk"), None),
            P(None, "blk"),
            P("dp", "blk"),
            P("blk", "dp"),
            P(),
            P(),
            P(),
            P(("dp", "blk"), None),
            P(("dp", "blk")),
            P(("dp", "blk"), None),
        ),
        out_specs=(P(("dp", "blk"), None), P(), P()),
        check_vma=False,
    )
```

```python
import jax
import jax.numpy as jnp
from jax import lax
from jax.experimental import pallas as pl
from jax.experimental.pallas import tpu as pltpu
from jax.sharding import PartitionSpec as P

MESH = pl.DeviceIdType.MESH
BF, F32 = jnp.bfloat16, jnp.float32

REL = (0, 1, 3, 2)
LINK_RATE, PAIR_RATE = 46.6e3, 300e3
HOP, PAIR_HOP = 1.8, 1.0
AHEAD = 2.5
GRAD_RANK = 50
SLOTS = 3


COPY_RANKS = (
    -1035, -564, -297, -1186, 1297, -323, 83, -1833, 1126, 2034, 74, 1002, -117, -115, -1310, 2730, -2076, -686, 1585, 164, 950, -354, 945, 1560,
    -262, 1893, 573, -2310, -928, 441, -1189, -117, -688, 2744, 995, 3082, 29, 1463, 411, -1001, -1815, 1111, 167, -1630, -161, -105, 1228, 805,
    337, -717, -300, 1439, -1755, -1329, 1111, -245, -427, -477, -193, 397, 409, 915, 1009, -310, -571, -1651, -684, -542, 459, -1420, 227, -1145,
    290, 2251, 1456, -337, 2771, 2945, 3560, 2121, 232, -953, -1179, 495, 1369, 110, -1722, -1659, 1144, 630, 2707, -270, -1954, 461, 703, -999,
    -562, -908, 1400, 1249, 534, -173, -2003, -144, -787, 363, -21, -1398, 1473, 27, 714, 433, -741, 470, 1795, -1568, 727, -969, -721, -177,
    -1276, -13, 2564, 3224, 39, 620, 1402, -962, -1736, 715, 785, 1952, 934, -1287, -1151, 1553, 807, -1691, 209, 2356, 466, -1055, 533, -106,
    931, 2818, -2301, 1912, 2921, -956, 195, 1857, 2449, 1351, 683, 623, 620, 1382, -1203, 580, -344, 58, 328, 63, 1143, 498, -1147, 13,
    810, 1313, 256, -132, -421, -674, 946, 1349, 226, 1417, 209, 320, 314, 43, 917, -362, 1870, -1583, -1719, -301, 615, -1421, -106, 655,
    652, -898, -451, 85, -650, 855, 1004, 800, 273, -2679, 553, 1105, 1057, -175, 284, -1020, -118, 1689, 1643, -206, 1655, 322, -1652, 325,
    -334, 1821, -332, -622, 1228, 2296,
)
TASK_RANKS = (
    -33, -1131, 1174, 1480, 1485, -2499, 257, -1955, -430, 1137, 287, 345, -2437, -385, 2439, 2912, -415, -1261, 1884, -1054, 293, 2581, -656, -5095,
    -347, 524, -2374, 2182, 455, 1020, -366, -2587, -2489, -622, -2566, -321, -3481, -4440, -106, -5293, 1667, -2396, 591, 294, -1230, 1401, -721, 171,
    1110, 385, -1132, -2307, -715, 1876, 2225, -1705, -2537, 662, 699, 2304, 192, 905, 475, 828, -1543, 2065, 417, 2995, 1855, -1717, -2158, -210,
    3577, 2676, -837, 944, 1596, 2779, -2082, -811, 414, 398, -425, 778, -633, 1703, 792, -1676, -656, 1519, 1951, 206, 1324, 1066, -56, -2582,
    -239, 2270, -2355, 2041, -637, 606, 1027, 1011, 158, 2195, 194, 2230, -4962, 2123, 476, 170, 2020, 1369, -1719, -1455, 2186, 850, -1015, 506,
    997, -1799, 754, -543, 1685, -2714, -393, -975, -237, 74, 1887, 2352,
)


class Copy:
    def __init__(self, name, link, size, source, landing, here, rank):
        self.name, self.link, self.size, self.rank = name, link, size, rank
        self.source, self.landing, self.here = source, landing, here
        self.after = set()


class Task:
    def __init__(self, name, cost, run, after, rank):
        self.name, self.cost, self.run, self.after, self.rank = name, cost, run, set(after), rank


def arrange(copies, tasks, begun):
    order, done, now = [], set(begun), 0.0
    free, arriving, queued = {}, [], {}
    to_send, to_run = list(copies), list(tasks)

    def send(copy):
        order.append(("send", copy))
        rate, hop = (PAIR_RATE, PAIR_HOP) if copy.link == "pair" else (LINK_RATE, HOP)
        start = max(now, free.get(copy.link, 0.0))
        free[copy.link] = end = start + copy.size / rate
        arriving.append((end + hop, copy))

    def send_ready(until):
        for copy in list(to_send):
            if copy.after <= done:
                to_send.remove(copy)
                queued.setdefault(copy.link, []).append(copy)
        for link, line in queued.items():
            line.sort(key=lambda copy: copy.rank)
            while line and (free.get(link, 0.0) < until or link == "pair"):
                send(line.pop(0))

    send_ready(AHEAD)
    while arriving or to_run:
        arriving.sort(key=lambda pair: pair[0])
        ready = [task for task in to_run if task.after <= done]
        if arriving and arriving[0][0] <= now:
            copy = arriving.pop(0)[1]
            order.append(("recv", copy))
            done.add(copy.name)
            send_ready(now + AHEAD)
        elif ready:
            task = min(ready, key=lambda task: task.rank)
            to_run.remove(task)
            order.append(("task", task))
            now += task.cost
            done.add(task.name)
            send_ready(now + AHEAD)
        else:
            send_ready(arriving[0][0] + AHEAD)
            arriving.sort(key=lambda pair: pair[0])
            now = arriving[0][0]
    assert not to_send
    return order, now


def kernel(tokens, gate, up, down, cotangent, factors_down, factors_up, router, routes, mask, base, grads_low, grads_high, tok, gw, ub, db, gact, uact, hid, psib, rsib, summed,
           rl, rr, fl, fr, ustage, dstage, g, stage, cot, fdown, fup, coef, scaled, turned, rz, rm, xs, ga, gb, load_sem, send_sem, recv_sem):
    dp, blk = lax.axis_index("dp"), lax.axis_index("blk")
    z, y, xh = dp // 8, (dp // 2) % 4, dp % 2
    xl, core = blk // 2, blk % 2
    x = xh * 2 + xl

    def device(dz=0, dy=0, dx=0, dc=0):
        at_z, at_y, at_x = (z + dz) % 4, (y + dy) % 4, (x + dx) % 4
        return ((at_z * 4 + at_y) * 2 + at_x // 2, (at_x % 2) * 2 + (core + dc) % 2)

    targets = {
        "z+": device(dz=1), "z-": device(dz=3), "y+": device(dy=1), "y-": device(dy=3),
        "x+": device(dx=1), "x-": device(dx=3), "pair": device(dc=1),
    }

    def plane(dz, dy):
        return ((z + dz) % 4) * 4 + (y + dy) % 4

    copies = []

    def add(name, link, size, source, landing, here, after=(), rank=0):
        copy = Copy(name, link, size, source, landing, here, rank)
        copy.after = set(after)
        copies.append(copy)
        return copy

    piece = 128 * 896 * 2

    def weight(kind, dz, dy, own, half=None):
        ref, rows = (ub, 128) if kind == "u" else (db, 896)
        ref = ref.at[plane(dz, dy), xh if own else 1 - xh]
        if half is None:
            return ref
        return ref.at[pl.ds(half * (rows // 2), rows // 2)]

    def spread(tag, ref, size, first, origin, base_rank):
        second = "z" if first == "y" else "y"

        def at(f, s, half=None):
            return ref(f, s, half) if first == "z" else ref(s, f, half)

        def move(name, link, f, s, f_new, s_new, after, rank, half=None):
            amount = size if half is None else size // 2
            add(tag + name, link, amount, at(f, s, half), at(f, s, half), at(f_new, s_new, half), after, rank + base_rank)

        move("F+", first + "+", 0, 0, 3, 0, origin, 0)
        move("F-", first + "-", 0, 0, 1, 0, origin, 0)
        move("S+0", second + "+", 0, 0, 0, 3, origin, 1)
        move("S-0", second + "-", 0, 0, 0, 1, origin, 1)
        move("G+", first + "+", 3, 0, 2, 0, [tag + "F+"], 2, 0)
        move("G-", first + "-", 1, 0, 2, 0, [tag + "F-"], 2, 1)
        came = {0: origin, 3: [tag + "F+"], 1: [tag + "F-"], 2: [tag + "G+", tag + "G-"]}
        for f in REL[1:]:
            move("S+%d" % f, second + "+", f, 0, f, 3, came[f], 4 if f == 2 else 3)
            move("S-%d" % f, second + "-", f, 0, f, 1, came[f], 4 if f == 2 else 3)
        for f in (0, 1):
            move("T+%d" % f, second + "+", f, 3, f, 2, [tag + "S+%d" % f], 5)
        for f in (3, 2):
            move("T-%d" % f, second + "-", f, 1, f, 2, [tag + "S-%d" % f], 5)

        def have(f, s):
            if s == 0:
                return came[f]
            if s == 3:
                return [tag + "S+%d" % f]
            if s == 1:
                return [tag + "S-%d" % f]
            return [tag + ("T+%d" if f in (0, 1) else "T-%d") % f]

        return (lambda dz, dy: have(dz, dy)) if first == "z" else (lambda dz, dy: have(dy, dz))

    def across(kind, hbm, ref, stage, rows, rank):
        for sign, step, half in (("+", 1, 0), ("-", 3, 1)):
            part = pl.ds(half * rows, rows)
            if kind == "u":
                source = hbm.at[part, pl.ds(pl.multiple_of((1 - xh) * 896, 128), 896)]
            else:
                source = hbm.at[pl.ds(pl.multiple_of((1 - xh) * 896 + half * rows, 64), rows), :]
            next_half = 1 - ((x + step) % 4) // 2
            hold = stage.at[half]
            add("A" + kind + sign, "x" + sign, piece // 2, source, hold, hold, [], rank)
            add("B" + kind + sign, "x" + sign, piece // 2, hold, ref.at[plane(0, 0), next_half, part],
                ref.at[plane(0, 0), 1 - xh, part], ["A" + kind + sign], rank)
        return ["B" + kind + "+", "B" + kind + "-"]

    mib = 128 * 4096 * 2
    have_au = across("u", up, ub, ustage, 64, 0)
    def columns_of(dz):
        return pl.ds(pl.multiple_of(((z + dz) % 4) * 1024, 1024), 1024)

    def some(r, c, dz):
        return tok.at[r, c, :, columns_of(dz)]

    came_tok = {}
    for dz in REL:
        came_tok[0, dz] = ["L"]
        for sign, r in (("+", 3), ("-", 1)):
            add("K%s%d" % (sign, dz), "x" + sign, mib // 4, some(0, 0, dz), some(r, 0, dz), some(r, 0, dz), ["L", "Au" + sign], 3)
            came_tok[r, dz] = ["K%s%d" % (sign, dz)]
        sign, r = ("+", 3) if dz < 2 else ("-", 1)
        add("KF%d" % dz, "x" + sign, mib // 4, some(r, 0, dz), some(2, 0, dz), some(2, 0, dz), came_tok[r, dz], 4)
        came_tok[2, dz] = ["KF%d" % dz]
        for r in REL:
            add("KS%d%d" % (r, dz), "pair", mib // 4, some(r, 0, dz), some(r, 1, dz), some(r, 1, dz), came_tok[r, dz])
            came_tok[r, dz] = came_tok[r, dz] + ["KS%d%d" % (r, dz)]
    have_ad = across("d", down, db, dstage, 448, 5)
    def piece_of(kind, own):
        return lambda dz, dy, half: weight(kind, dz, dy, own, half)

    have_uo = spread("uo", piece_of("u", True), piece, "y", ["L"], 0)
    have_up = spread("up", piece_of("u", False), piece, "z", have_au, 0)
    have_do = spread("do", piece_of("d", True), piece, "z", ["L"], 100)
    have_dp = spread("dp", piece_of("d", False), piece, "y", have_ad, 100)

    tasks = []

    def run_gate(places, n, dz):
        def run():
            def step(i, carry):
                k = pl.multiple_of(((z + dz) % 4) * 1024 + i * 512, 512)
                left = jnp.concatenate([tok[r, :, :, pl.ds(k, 512)].reshape(256, 512) for r in places], axis=0)
                part = jnp.dot(left, gw[pl.ds(k, 512), :], preferred_element_type=F32)
                for m, r in enumerate(places):
                    gact[r] += part[m * 256:m * 256 + 256]
                return carry

            if n == 0:
                for r in places:
                    gact[r] = jnp.zeros((256, 896), F32)
                    uact[r] = jnp.zeros((256, 896), F32)
            lax.fori_loop(0, 2, step, 0)
            if n == 3:
                for r in places:
                    v = gact[r]
                    gact[r] = v / (1.0 + jnp.exp(-v))
        return run

    def run_up(dz, dy, i):
        def run():
            j = plane(dz, dy)
            columns = pl.ds(pl.multiple_of(j * 256, 256), 256)
            two = pl.ds(i * 2, 2)
            left = tok[two, :, :, columns].reshape(512, 256)
            part = jnp.dot(left, ub[j].reshape(256, 896), preferred_element_type=F32)
            uact[two] += part.reshape(2, 256, 896)
        return run

    def run_hidden():
        hid[...] = (gact[...] * uact[...]).astype(BF)

    ups = []
    for name, cost, places in (("G0", 1.4, (0,)), ("G1", 2.2, (1, 3)), ("G2", 1.4, (2,))):
        for n, dz in enumerate(REL):
            ready = [name + str(n - 1)] if n else ["LG"]
            tasks.append(Task(name + str(n), cost, run_gate(places, n, dz), ready + [m for r in places for m in came_tok[r, dz]], 10))
    ups = ["G03", "G13", "G23"]
    for dz in REL:
        for dy in REL:
            for i in (0, 1):
                ready = have_uo(dz, dy) + have_up(dz, dy) + ["G10", "G20" if i else "G00"]
                ready = ready + [m for r in (2 * i, 2 * i + 1) for m in came_tok[r, dz]]
                ups.append("U%d%d%d" % (dz, dy, i))
                tasks.append(Task(ups[-1], 0.45, run_up(dz, dy, i), ready, 20 + i))
    tasks.append(Task("H", 0.5, run_hidden, ups, 0))
    blocks = sorted(((dz, dy) for dz in range(4) for dy in range(4)), key=lambda p: (min(p[0], 4 - p[0]) + min(p[1], 4 - p[1]), p))
    size = 128 * 256 * 2

    slot = {}

    def run_down(b, dz, dy):
        def run():
            j = plane(dz, dy)

            def step(i, carry):
                right = jnp.concatenate([db[j, 0], db[j, 1]], axis=1)
                left = hid[pl.ds(i * 2, 2)].reshape(512, 896)
                part = jnp.dot(left, right, preferred_element_type=F32).astype(BF).reshape(2, 2, 128, 256)
                summed[b, pl.ds(i * 2, 2)] = part[:, 0]
                psib[slot[b], pl.ds(i * 2, 2)] = part[:, 1]
                return carry

            lax.fori_loop(0, 2, step, 0)
        return run

    def run_add(b):
        def run():
            summed[b] = (summed[b].astype(F32) + rsib[b].astype(F32)).astype(BF)
        return run

    def run_merge(b):
        def run():
            if b % 2 == 0:
                summed[b, 1] = (summed[b, 1].astype(F32) + rl[b // 2].astype(F32)).astype(BF)
            else:
                summed[b, 3] = (summed[b, 3].astype(F32) + rr[b // 2].astype(F32)).astype(BF)
        return run

    def run_final(b, dz, dy):
        def run():
            total = summed[b, 0].astype(F32) + fl[b].astype(F32) + fr[b].astype(F32)
            columns = pl.ds(pl.multiple_of(plane(dz, dy) * 256, 256), 256)
            delta = jnp.dot(scaled[...], fup[:, columns], preferred_element_type=F32)
            base[:, columns] = (total + delta).astype(BF)
        return run

    hidden = ["H"]
    for b, (dz, dy) in enumerate(blocks):
        n, half = str(b), b // 2
        tasks.append(Task("D" + n, 1.25, run_down(b, dz, dy), hidden + have_do(dz, dy) + have_dp(dz, dy), 300 + b))
        add("Q" + n, "pair", 4 * size, None, rsib.at[b], rsib.at[b], ["D" + n])
        tasks.append(Task("A" + n, 0.15, run_add(b), ["D" + n, "Q" + n], 200 + b))
        if b % 2 == 0:
            add("Z" + n, "x+", size, summed.at[b, 2], rl.at[half], rl.at[half], ["A" + n], 10 + 3 * b)
            add("N" + n, "x-", size, summed.at[b, 3], fr.at[b], fr.at[b], ["A" + n], 12 + 3 * b)
            add("M" + n, "x+", size, summed.at[b, 1], fl.at[b], fl.at[b], ["C" + n], 11 + 3 * b)
        else:
            add("Z" + n, "x-", size, summed.at[b, 2], rr.at[half], rr.at[half], ["A" + n], 10 + 3 * b)
            add("N" + n, "x+", size, summed.at[b, 1], fl.at[b], fl.at[b], ["A" + n], 12 + 3 * b)
            add("M" + n, "x-", size, summed.at[b, 3], fr.at[b], fr.at[b], ["C" + n], 11 + 3 * b)
        tasks.append(Task("C" + n, 0.05, run_merge(b), ["A" + n, "Z" + n], 100 + b))
        tasks.append(Task("E" + n, 0.2, run_final(b, dz, dy), ["A" + n, "M" + n, "N" + n, "W0"], 400 + b))

    wide = 1152 * 4

    def upright(row):
        return jnp.broadcast_to(row.astype(F32), (128, 128)).T

    def run_low():
        mine = tok[0, 0]
        across = (((1,), (1,)), ((), ()))
        logits = lax.dot_general(mine, router[...], across, preferred_element_type=F32)
        first, second = upright(routes[0:1, :]), upright(routes[1:2, :])
        expert = lax.broadcasted_iota(jnp.int32, (128, 8), 1).astype(F32)
        first_logit = jnp.sum(jnp.where(expert == first[:, 0:8], logits, 0.0), axis=1, keepdims=True)
        second_logit = jnp.sum(jnp.where(expert == second[:, 0:8], logits, 0.0), axis=1, keepdims=True)
        weight = jax.nn.sigmoid(first_logit - second_logit)
        column = (lax.broadcasted_iota(jnp.int32, (128, 128), 1) // 16).astype(F32)
        wide_coef = jnp.where(column == first, weight, jnp.where(column == second, 1.0 - weight, 0.0))
        coef[...] = wide_coef
        low = jnp.dot(mine, fdown[...], preferred_element_type=F32)
        value = (low * wide_coef).astype(BF)
        scaled[...] = value
        turned[1] = value.astype(F32).T.astype(BF)

    def run_dlow():
        cot[...] = cot[...] * upright(mask[...])[:, 0:1].astype(BF)
        low = lax.dot_general(cot[...], fup[...], (((1,), (1,)), ((), ())), preferred_element_type=F32)
        turned[0] = (low * coef[...]).astype(BF).astype(F32).T.astype(BF)

    def local_part(owner, ab, h):
        columns = pl.ds(pl.multiple_of(owner * 2048 + ab * 1024, 1024), 1024)
        right = cot[:, columns] if h else tok[0, 0, :, columns]
        return jnp.dot(turned[h], right, preferred_element_type=F32)

    def count():
        return jnp.broadcast_to(jnp.sum(mask[...].astype(F32), axis=1, keepdims=True), (128, 128))

    tasks.append(Task("W0", 3.5, run_low, ["L", "LC"], 3))
    tasks.append(Task("W1", 2.5, run_dlow, ["W0"], 3))
    pieces = [(ab, h) for ab in range(2) for h in range(2)]
    for n, (ab, h) in enumerate(pieces):
        name = "PG%d%d" % (ab, h)

        def run_theirs(n=n, ab=ab, h=h):
            if n >= 2:
                early = by_name["PG%d%d" % pieces[n - 2]]
                descriptor(early, early.landing).wait_send()
            stage[n % 2, :, 0:1024] = local_part(1 - core, ab, h)
            stage[n % 2, :, 1024:1152] = count()

        def run_ours(ab=ab, h=h):
            rows = slice(h * 128, h * 128 + 128)
            g[ab, rows, 0:1024] += local_part(core, ab, h)
            g[ab, rows, 1024:1152] += count()

        landing = g.at[ab, pl.ds(h * 128, 128)]
        tasks.append(Task("WS%d%d" % (ab, h), 0.5, run_theirs, ["W1"] + (["WS%d%d" % pieces[n - 1]] if n else []), 3))
        add(name, "pair", 128 * wide, stage.at[n % 2], landing, landing, ["WS%d%d" % (ab, h)], 1)
        tasks.append(Task("WO%d%d" % (ab, h), 0.5, run_ours, [name, "W1"], 4))

    def reduce_ring(tag, axis, piece_at, hold_z, hold_m, rows, after, finish, rank):
        amount = rows * wide
        for sign, near, half in (("+", 1, 0), ("-", 3, 1)):
            add(tag + "Z" + sign, axis + sign, amount // 2, piece_at(2, half), hold_z.at[half], hold_z.at[half], after, rank)

            def combine(near=near, half=half):
                ref = piece_at(near, half)
                ref[...] = ref[...] + hold_z[half]

            tasks.append(Task(tag + "C" + sign, 0.2, combine, after + [tag + "Z" + sign], 6))
            add(tag + "M" + sign, axis + sign, amount, piece_at(near), hold_m.at[half], hold_m.at[half], [tag + "C" + sign], rank)
        tasks.append(Task(tag + "E", 0.3, finish, after + [tag + "M+", tag + "M-"], 6))

    row_of = {"y": y, "z": z}
    for ab, (first, second) in enumerate((("y", "z"), ("z", "y"))):
        p, q = row_of[first], row_of[second]

        def block(d, half=None, ab=ab, p=p):
            rows = pl.multiple_of(((p + d) % 4) * 64 + (half or 0) * 32, 32)
            return g.at[ab, pl.ds(rows, 64 if half is None else 32)]

        def slim(d, half=None, ab=ab, p=p, q=q):
            rows = pl.multiple_of(p * 64 + ((q + d) % 4) * 16 + (half or 0) * 8, 8)
            return g.at[ab, pl.ds(rows, 16 if half is None else 8)]

        z1, m1 = rz.at[ab, :, pl.ds(0, 32)], rm.at[ab, :, pl.ds(0, 64)]
        z2, m2 = rz.at[ab, :, pl.ds(32, 8)], rm.at[ab, :, pl.ds(64, 16)]

        def first_done(block=block, ab=ab):
            ref = block(0)
            ref[...] = ref[...] + rm[ab, 0, 0:64] + rm[ab, 1, 0:64]

        def second_done(slim=slim, ab=ab):
            xs[0, ab] = slim(0)[...] + rm[ab, 0, 64:80] + rm[ab, 1, 64:80]

        reduce_ring("R%d" % ab, first, block, z1, m1, 64, ["WO%d0" % ab, "WO%d1" % ab], first_done, GRAD_RANK)
        reduce_ring("S%d" % ab, second, slim, z2, m2, 16, ["R%dE" % ab], second_done, GRAD_RANK)

    slices = ["S0E", "S1E"]
    add("X+", "x+", 32 * wide, xs.at[0], xs.at[3], xs.at[3], slices, 6)
    add("X-", "x-", 32 * wide, xs.at[0], xs.at[1], xs.at[1], slices, 6)
    add("XF+", "x+", 16 * wide, xs.at[3, 0], xs.at[2, 0], xs.at[2, 0], ["X+"], 6)
    add("XF-", "x-", 16 * wide, xs.at[1, 1], xs.at[2, 1], xs.at[2, 1], ["X-"], 6)

    def row_block(ab, dz, dy):
        at_z, at_y = (z + dz) % 4, (y + dy) % 4
        return at_z * 4 + at_y if ab else at_y * 4 + at_z

    def run_whole():
        for ab in range(2):
            total = (xs[0, ab] + xs[2, ab]) + (xs[1, ab] + xs[3, ab])
            inverse = 1.0 / jnp.maximum(total[:, 1024:1025], 1.0)
            ga[ab, row_block(ab, 0, 0)] = (total[:, 0:1024] * inverse).astype(BF)

    tasks.append(Task("XS", 0.4, run_whole, slices + ["X+", "X-", "XF+", "XF-"], 6))
    for ab, first in enumerate("yz"):
        def finished(dz, dy, half, ab=ab):
            ref = ga.at[ab, row_block(ab, dz, dy)]
            return ref if half is None else ref.at[:, pl.ds(half * 512, 512)]

        have = spread("g%d" % ab, finished, 16 * 1024 * 2, first, ["XS"], GRAD_RANK)
        whole = sorted({n for dz in range(4) for dy in range(4) for n in have(dz, dy)})
        add("PH%d" % ab, "pair", 256 * 1024 * 2, ga.at[ab], gb.at[ab], gb.at[ab], whole)

    for item, rank in zip(copies + tasks, COPY_RANKS + TASK_RANKS, strict=True):
        item.rank = rank
    for item, rank in zip(copies + tasks, COPY_RANKS + TASK_RANKS, strict=True):
        item.rank = rank
    order, _ = arrange(copies, tasks, ["L", "LG", "LC"])
    assert len(copies) == COPIES
    place = {copy.name: i for i, copy in enumerate(copies)}
    by_name = {copy.name: copy for copy in copies}

    def descriptor(copy, landing):
        i = place[copy.name]
        return pltpu.make_async_remote_copy(
            src_ref=copy.source, dst_ref=landing, send_sem=send_sem.at[i], recv_sem=recv_sem.at[i],
            device_id=targets[copy.link], device_id_type=MESH)

    loads = [
        pltpu.make_async_copy(tokens, tok.at[0, 0], load_sem.at[0]),
        pltpu.make_async_copy(up.at[:, pl.ds(pl.multiple_of(xh * 896, 128), 896)], ub.at[plane(0, 0), xh], load_sem.at[1]),
        pltpu.make_async_copy(down.at[pl.ds(pl.multiple_of(xh * 896, 128), 896), :], db.at[plane(0, 0), xh], load_sem.at[2]),
    ]
    load_gate = pltpu.make_async_copy(gate.at[:, pl.ds(pl.multiple_of(xh * 896, 128), 896)], gw, load_sem.at[3])
    extra = [
        pltpu.make_async_copy(cotangent, cot, load_sem.at[4]),
        pltpu.make_async_copy(factors_down, fdown, load_sem.at[5]),
        pltpu.make_async_copy(factors_up, fup, load_sem.at[6]),
    ]
    for load in loads:
        load.start()
    for load in extra:
        load.start()
    load_gate.start()
    barrier = pltpu.get_barrier_semaphore()
    for target in targets.values():
        pl.semaphore_signal(barrier, inc=1, device_id=target, device_id_type=MESH)
    pl.semaphore_wait(barrier, len(targets))
    for load in loads:
        load.wait()
    gate_waited = False
    used = []
    for what, item in order:
        if item.name[0] == "D" and what == "task":
            if len(used) >= SLOTS:
                early = by_name["Q" + used[-SLOTS]]
                descriptor(early, early.landing).wait_send()
            slot[int(item.name[1:])] = len(used) % SLOTS
            used.append(item.name[1:])
            by_name["Q" + used[-1]].source = psib.at[slot[int(used[-1])]]
        if what == "send":
            descriptor(item, item.landing).start()
        elif what == "recv":
            descriptor(item, item.here).wait_recv()
        else:
            if item.name[0] == "G" and not gate_waited:
                load_gate.wait()
                gate_waited = True
            if item.name == "W0":
                for load in extra:
                    load.wait()
            item.run()
    stores = []
    for half, whole in ((core, ga), (1 - core, gb)):
        for ab in range(2):
            columns = pl.ds(pl.multiple_of(half * 2048 + ab * 1024, 1024), 1024)
            for n, result in enumerate((grads_low, grads_high)):
                part = whole.at[ab, pl.ds(8 * n, 8)]
                stores.append(pltpu.make_async_copy(part, result.at[:, :, columns], load_sem.at[len(stores)]))
    for store in stores:
        store.start()
    already = {"Q" + n for n in used[:-SLOTS]} | {"PG00", "PG01"}
    for copy in copies:
        if copy.name not in already:
            descriptor(copy, copy.landing).wait_send()
    for store in stores:
        store.wait()


COPIES = 8 + 28 + 64 + 64 + 4 + 16 + 4 + 32 + 2


def layer(*operands):
    hbm = pl.BlockSpec(memory_space=pl.ANY)
    return pl.pallas_call(
        kernel,
        out_shape=(jax.ShapeDtypeStruct((128, 4096), BF), jax.ShapeDtypeStruct((8, 16, 4096), BF), jax.ShapeDtypeStruct((8, 16, 4096), BF)),
        in_specs=[hbm] * 7 + [pl.BlockSpec(memory_space=pltpu.VMEM)] * 3,
        out_specs=(pl.BlockSpec(memory_space=pltpu.VMEM), hbm, hbm),
        scratch_shapes=[
            pltpu.VMEM((4, 2, 128, 4096), BF),
            pltpu.VMEM((4096, 896), BF),
            pltpu.VMEM((16, 2, 128, 896), BF),
            pltpu.VMEM((16, 2, 896, 128), BF),
            pltpu.VMEM((4, 256, 896), F32),
            pltpu.VMEM((4, 256, 896), F32),
            pltpu.VMEM((4, 256, 896), BF),
            pltpu.VMEM((SLOTS, 4, 128, 256), BF),
            pltpu.VMEM((16, 4, 128, 256), BF),
            pltpu.VMEM((16, 4, 128, 256), BF),
            pltpu.VMEM((8, 128, 256), BF),
            pltpu.VMEM((8, 128, 256), BF),
            pltpu.VMEM((16, 128, 256), BF),
            pltpu.VMEM((16, 128, 256), BF),
            pltpu.VMEM((2, 64, 896), BF),
            pltpu.VMEM((2, 448, 128), BF),
            pltpu.VMEM((2, 256, 1152), F32),
            pltpu.VMEM((2, 128, 1152), F32),
            pltpu.VMEM((128, 4096), BF),
            pltpu.VMEM((4096, 128), BF),
            pltpu.VMEM((128, 4096), BF),
            pltpu.VMEM((128, 128), F32),
            pltpu.VMEM((128, 128), BF),
            pltpu.VMEM((2, 128, 128), BF),
            pltpu.VMEM((2, 2, 40, 1152), F32),
            pltpu.VMEM((2, 2, 80, 1152), F32),
            pltpu.VMEM((4, 2, 16, 1152), F32),
            pltpu.VMEM((2, 16, 16, 1024), BF),
            pltpu.VMEM((2, 16, 16, 1024), BF),
            pltpu.SemaphoreType.DMA((8,)),
            pltpu.SemaphoreType.DMA((COPIES,)),
            pltpu.SemaphoreType.DMA((COPIES,)),
        ],
        compiler_params=pltpu.CompilerParams(
            collective_id=0, has_side_effects=True, vmem_limit_bytes=67_000_000),
        cost_estimate=pl.CostEstimate(flops=22_500_000_000, bytes_accessed=16_000_000, transcendentals=1_000_000),
        name="layer",
    )(*operands)


def shards(
    tokens,
    gate_projection_weight,
    up_projection_weight,
    down_projection_weight,
    router_projection_weight,
    adapter_down_factors,
    adapter_up_factors,
    routes,
    padding_token_mask,
    cotangent,
):
    layer_out, grads_low, grads_high = layer(
        tokens, gate_projection_weight, up_projection_weight, down_projection_weight,
        cotangent, adapter_down_factors, adapter_up_factors, router_projection_weight.T, routes.T,
        padding_token_mask[None, :])
    unit = jnp.eye(128, dtype=BF)
    grad_down = lax.dot_general(grads_low.reshape(128, 4096), unit, (((0,), (0,)), ((), ())), preferred_element_type=F32)
    grad_up = grads_high.reshape(128, 4096).astype(F32)
    return (layer_out, grad_down, grad_up)


def solution(mesh):
    return jax.shard_map(
        shards,
        mesh=mesh,
        in_specs=(
            P(("dp", "blk"), None),
            P(None, "blk"),
            P("dp", "blk"),
            P("blk", "dp"),
            P(),
            P(),
            P(),
            P(("dp", "blk"), None),
            P(("dp", "blk")),
            P(("dp", "blk"), None),
        ),
        out_specs=(P(("dp", "blk"), None), P(), P()),
        check_vma=False,
    )
```

```python
import jax
import jax.numpy as jnp
from jax import lax
from jax.experimental import pallas as pl
from jax.experimental.pallas import tpu as pltpu
from jax.sharding import PartitionSpec as P

MESH = pl.DeviceIdType.MESH
BF, F32 = jnp.bfloat16, jnp.float32

REL = (0, 1, 3, 2)
LINK_RATE, PAIR_RATE = 46.6e3, 300e3
HOP, PAIR_HOP = 1.8, 1.0
AHEAD = 2.5
GRAD_RANK = 50
SLOTS = 3


COPY_RANKS = (
    -1035, -564, -297, -1186, 1297, -323, 83, -1833, 1126, 2034, 74, 1002, -117, -115, -1310, 2730, -2076, -686, 1585, 164, 950, -354, 945, 1560,
    -262, 1893, 573, -2310, -928, 441, -1189, -117, -688, 2744, 995, 3082, 29, 1463, 411, -1001, -1815, 1111, 167, -1630, -161, -105, 1228, 805,
    337, -717, -300, 1439, -1755, -1329, 1111, -245, -427, -477, -193, 397, 409, 915, 1009, -310, -571, -1651, -684, -542, 459, -1420, 227, -1145,
    290, 2251, 1456, -337, 2771, 2945, 3560, 2121, 232, -953, -1179, 495, 1369, 110, -1722, -1659, 1144, 630, 2707, -270, -1954, 461, 703, -999,
    -562, -908, 1400, 1249, 534, -173, -2003, -144, -787, 363, -21, -1398, 1473, 27, 714, 433, -741, 470, 1795, -1568, 727, -969, -721, -177,
    -1276, -13, 2564, 3224, 39, 620, 1402, -962, -1736, 715, 785, 1952, 934, -1287, -1151, 1553, 807, -1691, 209, 2356, 466, -1055, 533, -106,
    931, 2818, -2301, 1912, 2921, -956, 195, 1857, 2449, 1351, 683, 623, 620, 1382, -1203, 580, -344, 58, 328, 63, 1143, 498, -1147, 13,
    810, 1313, 256, -132, -421, -674, 946, 1349, 226, 1417, 209, 320, 314, 43, 917, -362, 1870, -1583, -1719, -301, 615, -1421, -106, 655,
    652, -898, -451, 85, -650, 855, 1004, 800, 273, -2679, 553, 1105, 1057, -175, 284, -1020, -118, 1689, 1643, -206, 1655, 322, -1652, 325,
    -334, 1821, -332, -622, 1228, 2296,
)
TASK_RANKS = (
    -33, -1131, 1174, 1480, 1485, -2499, 257, -1955, -430, 1137, 287, 345, -2437, -385, 2439, 2912, -415, -1261, 1884, -1054, 293, 2581, -656, -5095,
    -347, 524, -2374, 2182, 455, 1020, -366, -2587, -2489, -622, -2566, -321, -3481, -4440, -106, -5293, 1667, -2396, 591, 294, -1230, 1401, -721, 171,
    1110, 385, -1132, -2307, -715, 1876, 2225, -1705, -2537, 662, 699, 2304, 192, 905, 475, 828, -1543, 2065, 417, 2995, 1855, -1717, -2158, -210,
    3577, 2676, -837, 944, 1596, 2779, -2082, -811, 414, 398, -425, 778, -633, 1703, 792, -1676, -656, 1519, 1951, 206, 1324, 1066, -56, -2582,
    -239, 2270, -2355, 2041, -637, 606, 1027, 1011, 158, 2195, 194, 2230, -4962, 2123, 476, 170, 2020, 1369, -1719, -1455, 2186, 850, -1015, 506,
    997, -1799, 754, -543, 1685, -2714, -393, -975, -237, 74, 1887, 2352,
)


class Copy:
    def __init__(self, name, link, size, source, landing, here, rank):
        self.name, self.link, self.size, self.rank = name, link, size, rank
        self.source, self.landing, self.here = source, landing, here
        self.after = set()


class Task:
    def __init__(self, name, cost, run, after, rank):
        self.name, self.cost, self.run, self.after, self.rank = name, cost, run, set(after), rank


def arrange(copies, tasks, begun):
    order, done, now = [], set(begun), 0.0
    free, arriving, queued = {}, [], {}
    to_send, to_run = list(copies), list(tasks)

    def send(copy):
        order.append(("send", copy))
        rate, hop = (PAIR_RATE, PAIR_HOP) if copy.link == "pair" else (LINK_RATE, HOP)
        start = max(now, free.get(copy.link, 0.0))
        free[copy.link] = end = start + copy.size / rate
        arriving.append((end + hop, copy))

    def send_ready(until):
        for copy in list(to_send):
            if copy.after <= done:
                to_send.remove(copy)
                queued.setdefault(copy.link, []).append(copy)
        for link, line in queued.items():
            line.sort(key=lambda copy: copy.rank)
            while line and (free.get(link, 0.0) < until or link == "pair"):
                send(line.pop(0))

    send_ready(AHEAD)
    while arriving or to_run:
        arriving.sort(key=lambda pair: pair[0])
        ready = [task for task in to_run if task.after <= done]
        if arriving and arriving[0][0] <= now:
            copy = arriving.pop(0)[1]
            order.append(("recv", copy))
            done.add(copy.name)
            send_ready(now + AHEAD)
        elif ready:
            task = min(ready, key=lambda task: task.rank)
            to_run.remove(task)
            order.append(("task", task))
            now += task.cost
            done.add(task.name)
            send_ready(now + AHEAD)
        else:
            send_ready(arriving[0][0] + AHEAD)
            arriving.sort(key=lambda pair: pair[0])
            now = arriving[0][0]
    assert not to_send
    return order, now


def kernel(tokens, gate, up, down, cotangent, factors_down, factors_up, router, routes, mask, base, grads_low, grads_high, tok, gw, ub, db, gact, uact, hid, psib, rsib, summed,
           rl, rr, fl, fr, ustage, dstage, g, stage, cot, fdown, fup, coef, scaled, turned, rz, rm, xs, ga, gb, load_sem, send_sem, recv_sem):
    dp, blk = lax.axis_index("dp"), lax.axis_index("blk")
    z, y, xh = dp // 8, (dp // 2) % 4, dp % 2
    xl, core = blk // 2, blk % 2
    x = xh * 2 + xl

    def device(dz=0, dy=0, dx=0, dc=0):
        at_z, at_y, at_x = (z + dz) % 4, (y + dy) % 4, (x + dx) % 4
        return ((at_z * 4 + at_y) * 2 + at_x // 2, (at_x % 2) * 2 + (core + dc) % 2)

    targets = {
        "z+": device(dz=1), "z-": device(dz=3), "y+": device(dy=1), "y-": device(dy=3),
        "x+": device(dx=1), "x-": device(dx=3), "pair": device(dc=1),
    }

    def plane(dz, dy):
        return ((z + dz) % 4) * 4 + (y + dy) % 4

    copies = []

    def add(name, link, size, source, landing, here, after=(), rank=0):
        copy = Copy(name, link, size, source, landing, here, rank)
        copy.after = set(after)
        copies.append(copy)
        return copy

    piece = 128 * 896 * 2

    def weight(kind, dz, dy, own, half=None):
        ref, rows = (ub, 128) if kind == "u" else (db, 896)
        ref = ref.at[plane(dz, dy), xh if own else 1 - xh]
        if half is None:
            return ref
        return ref.at[pl.ds(half * (rows // 2), rows // 2)]

    def spread(tag, ref, size, first, origin, base_rank):
        second = "z" if first == "y" else "y"

        def at(f, s, half=None):
            return ref(f, s, half) if first == "z" else ref(s, f, half)

        def move(name, link, f, s, f_new, s_new, after, rank, half=None):
            amount = size if half is None else size // 2
            add(tag + name, link, amount, at(f, s, half), at(f, s, half), at(f_new, s_new, half), after, rank + base_rank)

        move("F+", first + "+", 0, 0, 3, 0, origin, 0)
        move("F-", first + "-", 0, 0, 1, 0, origin, 0)
        move("S+0", second + "+", 0, 0, 0, 3, origin, 1)
        move("S-0", second + "-", 0, 0, 0, 1, origin, 1)
        move("G+", first + "+", 3, 0, 2, 0, [tag + "F+"], 2, 0)
        move("G-", first + "-", 1, 0, 2, 0, [tag + "F-"], 2, 1)
        came = {0: origin, 3: [tag + "F+"], 1: [tag + "F-"], 2: [tag + "G+", tag + "G-"]}
        for f in REL[1:]:
            move("S+%d" % f, second + "+", f, 0, f, 3, came[f], 4 if f == 2 else 3)
            move("S-%d" % f, second + "-", f, 0, f, 1, came[f], 4 if f == 2 else 3)
        for f in (0, 1):
            move("T+%d" % f, second + "+", f, 3, f, 2, [tag + "S+%d" % f], 5)
        for f in (3, 2):
            move("T-%d" % f, second + "-", f, 1, f, 2, [tag + "S-%d" % f], 5)

        def have(f, s):
            if s == 0:
                return came[f]
            if s == 3:
                return [tag + "S+%d" % f]
            if s == 1:
                return [tag + "S-%d" % f]
            return [tag + ("T+%d" if f in (0, 1) else "T-%d") % f]

        return (lambda dz, dy: have(dz, dy)) if first == "z" else (lambda dz, dy: have(dy, dz))

    def across(kind, hbm, ref, stage, rows, rank):
        for sign, step, half in (("+", 1, 0), ("-", 3, 1)):
            part = pl.ds(half * rows, rows)
            if kind == "u":
                source = hbm.at[part, pl.ds(pl.multiple_of((1 - xh) * 896, 128), 896)]
            else:
                source = hbm.at[pl.ds(pl.multiple_of((1 - xh) * 896 + half * rows, 64), rows), :]
            next_half = 1 - ((x + step) % 4) // 2
            hold = stage.at[half]
            add("A" + kind + sign, "x" + sign, piece // 2, source, hold, hold, [], rank)
            add("B" + kind + sign, "x" + sign, piece // 2, hold, ref.at[plane(0, 0), next_half, part],
                ref.at[plane(0, 0), 1 - xh, part], ["A" + kind + sign], rank)
        return ["B" + kind + "+", "B" + kind + "-"]

    mib = 128 * 4096 * 2
    have_au = across("u", up, ub, ustage, 64, 0)
    def columns_of(dz):
        return pl.ds(pl.multiple_of(((z + dz) % 4) * 1024, 1024), 1024)

    def some(r, c, dz):
        return tok.at[r, c, :, columns_of(dz)]

    came_tok = {}
    for dz in REL:
        came_tok[0, dz] = ["L"]
        for sign, r in (("+", 3), ("-", 1)):
            add("K%s%d" % (sign, dz), "x" + sign, mib // 4, some(0, 0, dz), some(r, 0, dz), some(r, 0, dz), ["L", "Au" + sign], 3)
            came_tok[r, dz] = ["K%s%d" % (sign, dz)]
        sign, r = ("+", 3) if dz < 2 else ("-", 1)
        add("KF%d" % dz, "x" + sign, mib // 4, some(r, 0, dz), some(2, 0, dz), some(2, 0, dz), came_tok[r, dz], 4)
        came_tok[2, dz] = ["KF%d" % dz]
        for r in REL:
            add("KS%d%d" % (r, dz), "pair", mib // 4, some(r, 0, dz), some(r, 1, dz), some(r, 1, dz), came_tok[r, dz])
            came_tok[r, dz] = came_tok[r, dz] + ["KS%d%d" % (r, dz)]
    have_ad = across("d", down, db, dstage, 448, 5)
    def piece_of(kind, own):
        return lambda dz, dy, half: weight(kind, dz, dy, own, half)

    have_uo = spread("uo", piece_of("u", True), piece, "y", ["L"], 0)
    have_up = spread("up", piece_of("u", False), piece, "z", have_au, 0)
    have_do = spread("do", piece_of("d", True), piece, "z", ["L"], 100)
    have_dp = spread("dp", piece_of("d", False), piece, "y", have_ad, 100)

    tasks = []

    def run_gate(places, n, dz):
        def run():
            def step(i, carry):
                k = pl.multiple_of(((z + dz) % 4) * 1024 + i * 512, 512)
                left = jnp.concatenate([tok[r, :, :, pl.ds(k, 512)].reshape(256, 512) for r in places], axis=0)
                part = jnp.dot(left, gw[pl.ds(k, 512), :], preferred_element_type=F32)
                for m, r in enumerate(places):
                    gact[r] += part[m * 256:m * 256 + 256]
                return carry

            if n == 0:
                for r in places:
                    gact[r] = jnp.zeros((256, 896), F32)
                    uact[r] = jnp.zeros((256, 896), F32)
            lax.fori_loop(0, 2, step, 0)
            if n == 3:
                for r in places:
                    v = gact[r]
                    gact[r] = v / (1.0 + jnp.exp(-v))
        return run

    def run_up(dz, dy, i):
        def run():
            j = plane(dz, dy)
            columns = pl.ds(pl.multiple_of(j * 256, 256), 256)
            two = pl.ds(i * 2, 2)
            left = tok[two, :, :, columns].reshape(512, 256)
            part = jnp.dot(left, ub[j].reshape(256, 896), preferred_element_type=F32)
            uact[two] += part.reshape(2, 256, 896)
        return run

    def run_hidden():
        hid[...] = (gact[...] * uact[...]).astype(BF)

    ups = []
    for name, cost, places in (("G0", 1.4, (0,)), ("G1", 2.2, (1, 3)), ("G2", 1.4, (2,))):
        for n, dz in enumerate(REL):
            ready = [name + str(n - 1)] if n else ["LG"]
            tasks.append(Task(name + str(n), cost, run_gate(places, n, dz), ready + [m for r in places for m in came_tok[r, dz]], 10))
    ups = ["G03", "G13", "G23"]
    for dz in REL:
        for dy in REL:
            for i in (0, 1):
                ready = have_uo(dz, dy) + have_up(dz, dy) + ["G10", "G20" if i else "G00"]
                ready = ready + [m for r in (2 * i, 2 * i + 1) for m in came_tok[r, dz]]
                ups.append("U%d%d%d" % (dz, dy, i))
                tasks.append(Task(ups[-1], 0.45, run_up(dz, dy, i), ready, 20 + i))
    tasks.append(Task("H", 0.5, run_hidden, ups, 0))
    blocks = sorted(((dz, dy) for dz in range(4) for dy in range(4)), key=lambda p: (min(p[0], 4 - p[0]) + min(p[1], 4 - p[1]), p))
    size = 128 * 256 * 2

    slot = {}

    def run_down(b, dz, dy):
        def run():
            j = plane(dz, dy)

            def step(i, carry):
                right = jnp.concatenate([db[j, 0], db[j, 1]], axis=1)
                left = hid[pl.ds(i * 2, 2)].reshape(512, 896)
                part = jnp.dot(left, right, preferred_element_type=F32).astype(BF).reshape(2, 2, 128, 256)
                summed[b, pl.ds(i * 2, 2)] = part[:, 0]
                psib[slot[b], pl.ds(i * 2, 2)] = part[:, 1]
                return carry

            lax.fori_loop(0, 2, step, 0)
        return run

    def run_add(b):
        def run():
            summed[b] = (summed[b].astype(F32) + rsib[b].astype(F32)).astype(BF)
        return run

    def run_merge(b):
        def run():
            if b % 2 == 0:
                summed[b, 1] = (summed[b, 1].astype(F32) + rl[b // 2].astype(F32)).astype(BF)
            else:
                summed[b, 3] = (summed[b, 3].astype(F32) + rr[b // 2].astype(F32)).astype(BF)
        return run

    def run_final(b, dz, dy):
        def run():
            total = summed[b, 0].astype(F32) + fl[b].astype(F32) + fr[b].astype(F32)
            columns = pl.ds(pl.multiple_of(plane(dz, dy) * 256, 256), 256)
            delta = jnp.dot(scaled[...], fup[:, columns], preferred_element_type=F32)
            base[:, columns] = (total + delta).astype(BF)
        return run

    hidden = ["H"]
    for b, (dz, dy) in enumerate(blocks):
        n, half = str(b), b // 2
        tasks.append(Task("D" + n, 1.25, run_down(b, dz, dy), hidden + have_do(dz, dy) + have_dp(dz, dy), 300 + b))
        add("Q" + n, "pair", 4 * size, None, rsib.at[b], rsib.at[b], ["D" + n])
        tasks.append(Task("A" + n, 0.15, run_add(b), ["D" + n, "Q" + n], 200 + b))
        if b % 2 == 0:
            add("Z" + n, "x+", size, summed.at[b, 2], rl.at[half], rl.at[half], ["A" + n], 10 + 3 * b)
            add("N" + n, "x-", size, summed.at[b, 3], fr.at[b], fr.at[b], ["A" + n], 12 + 3 * b)
            add("M" + n, "x+", size, summed.at[b, 1], fl.at[b], fl.at[b], ["C" + n], 11 + 3 * b)
        else:
            add("Z" + n, "x-", size, summed.at[b, 2], rr.at[half], rr.at[half], ["A" + n], 10 + 3 * b)
            add("N" + n, "x+", size, summed.at[b, 1], fl.at[b], fl.at[b], ["A" + n], 12 + 3 * b)
            add("M" + n, "x-", size, summed.at[b, 3], fr.at[b], fr.at[b], ["C" + n], 11 + 3 * b)
        tasks.append(Task("C" + n, 0.05, run_merge(b), ["A" + n, "Z" + n], 100 + b))
        tasks.append(Task("E" + n, 0.2, run_final(b, dz, dy), ["A" + n, "M" + n, "N" + n, "W0"], 400 + b))

    wide = 1152 * 4

    def upright(row):
        return jnp.broadcast_to(row.astype(F32), (128, 128)).T

    def run_low():
        mine = tok[0, 0]
        across = (((1,), (1,)), ((), ()))
        logits = lax.dot_general(mine, router[...], across, preferred_element_type=F32)
        first, second = upright(routes[0:1, :]), upright(routes[1:2, :])
        expert = lax.broadcasted_iota(jnp.int32, (128, 8), 1).astype(F32)
        first_logit = jnp.sum(jnp.where(expert == first[:, 0:8], logits, 0.0), axis=1, keepdims=True)
        second_logit = jnp.sum(jnp.where(expert == second[:, 0:8], logits, 0.0), axis=1, keepdims=True)
        weight = jax.nn.sigmoid(first_logit - second_logit)
        column = (lax.broadcasted_iota(jnp.int32, (128, 128), 1) // 16).astype(F32)
        wide_coef = jnp.where(column == first, weight, jnp.where(column == second, 1.0 - weight, 0.0))
        coef[...] = wide_coef
        low = jnp.dot(mine, fdown[...], preferred_element_type=F32)
        value = (low * wide_coef).astype(BF)
        scaled[...] = value
        turned[1] = value.astype(F32).T.astype(BF)

    def run_dlow():
        cot[...] = cot[...] * upright(mask[...])[:, 0:1].astype(BF)
        low = lax.dot_general(cot[...], fup[...], (((1,), (1,)), ((), ())), preferred_element_type=F32)
        turned[0] = (low * coef[...]).astype(BF).astype(F32).T.astype(BF)

    def local_part(owner, ab, h):
        columns = pl.ds(pl.multiple_of(owner * 2048 + ab * 1024, 1024), 1024)
        right = cot[:, columns] if h else tok[0, 0, :, columns]
        return jnp.dot(turned[h], right, preferred_element_type=F32)

    def count():
        return jnp.broadcast_to(jnp.sum(mask[...].astype(F32), axis=1, keepdims=True), (128, 128))

    tasks.append(Task("W0", 3.5, run_low, ["L", "LC"], 3))
    tasks.append(Task("W1", 2.5, run_dlow, ["W0"], 3))
    pieces = [(ab, h) for ab in range(2) for h in range(2)]
    for n, (ab, h) in enumerate(pieces):
        name = "PG%d%d" % (ab, h)

        def run_theirs(n=n, ab=ab, h=h):
            if n >= 2:
                early = by_name["PG%d%d" % pieces[n - 2]]
                descriptor(early, early.landing).wait_send()
            stage[n % 2, :, 0:1024] = local_part(1 - core, ab, h)
            stage[n % 2, :, 1024:1152] = count()

        def run_ours(ab=ab, h=h):
            rows = slice(h * 128, h * 128 + 128)
            g[ab, rows, 0:1024] += local_part(core, ab, h)
            g[ab, rows, 1024:1152] += count()

        landing = g.at[ab, pl.ds(h * 128, 128)]
        tasks.append(Task("WS%d%d" % (ab, h), 0.5, run_theirs, ["W1"] + (["WS%d%d" % pieces[n - 1]] if n else []), 3))
        add(name, "pair", 128 * wide, stage.at[n % 2], landing, landing, ["WS%d%d" % (ab, h)], 1)
        tasks.append(Task("WO%d%d" % (ab, h), 0.5, run_ours, [name, "W1"], 4))

    def reduce_ring(tag, axis, piece_at, hold_z, hold_m, rows, after, finish, rank):
        amount = rows * wide
        for sign, near, half in (("+", 1, 0), ("-", 3, 1)):
            add(tag + "Z" + sign, axis + sign, amount // 2, piece_at(2, half), hold_z.at[half], hold_z.at[half], after, rank)

            def combine(near=near, half=half):
                ref = piece_at(near, half)
                ref[...] = ref[...] + hold_z[half]

            tasks.append(Task(tag + "C" + sign, 0.2, combine, after + [tag + "Z" + sign], 6))
            add(tag + "M" + sign, axis + sign, amount, piece_at(near), hold_m.at[half], hold_m.at[half], [tag + "C" + sign], rank)
        tasks.append(Task(tag + "E", 0.3, finish, after + [tag + "M+", tag + "M-"], 6))

    row_of = {"y": y, "z": z}
    for ab, (first, second) in enumerate((("y", "z"), ("z", "y"))):
        p, q = row_of[first], row_of[second]

        def block(d, half=None, ab=ab, p=p):
            rows = pl.multiple_of(((p + d) % 4) * 64 + (half or 0) * 32, 32)
            return g.at[ab, pl.ds(rows, 64 if half is None else 32)]

        def slim(d, half=None, ab=ab, p=p, q=q):
            rows = pl.multiple_of(p * 64 + ((q + d) % 4) * 16 + (half or 0) * 8, 8)
            return g.at[ab, pl.ds(rows, 16 if half is None else 8)]

        z1, m1 = rz.at[ab, :, pl.ds(0, 32)], rm.at[ab, :, pl.ds(0, 64)]
        z2, m2 = rz.at[ab, :, pl.ds(32, 8)], rm.at[ab, :, pl.ds(64, 16)]

        def first_done(block=block, ab=ab):
            ref = block(0)
            ref[...] = ref[...] + rm[ab, 0, 0:64] + rm[ab, 1, 0:64]

        def second_done(slim=slim, ab=ab):
            xs[0, ab] = slim(0)[...] + rm[ab, 0, 64:80] + rm[ab, 1, 64:80]

        reduce_ring("R%d" % ab, first, block, z1, m1, 64, ["WO%d0" % ab, "WO%d1" % ab], first_done, GRAD_RANK)
        reduce_ring("S%d" % ab, second, slim, z2, m2, 16, ["R%dE" % ab], second_done, GRAD_RANK)

    slices = ["S0E", "S1E"]
    add("X+", "x+", 32 * wide, xs.at[0], xs.at[3], xs.at[3], slices, 6)
    add("X-", "x-", 32 * wide, xs.at[0], xs.at[1], xs.at[1], slices, 6)
    add("XF+", "x+", 16 * wide, xs.at[3, 0], xs.at[2, 0], xs.at[2, 0], ["X+"], 6)
    add("XF-", "x-", 16 * wide, xs.at[1, 1], xs.at[2, 1], xs.at[2, 1], ["X-"], 6)

    def row_block(ab, dz, dy):
        at_z, at_y = (z + dz) % 4, (y + dy) % 4
        return at_z * 4 + at_y if ab else at_y * 4 + at_z

    def run_whole():
        for ab in range(2):
            total = (xs[0, ab] + xs[2, ab]) + (xs[1, ab] + xs[3, ab])
            inverse = 1.0 / jnp.maximum(total[:, 1024:1025], 1.0)
            ga[ab, row_block(ab, 0, 0)] = (total[:, 0:1024] * inverse).astype(BF)

    tasks.append(Task("XS", 0.4, run_whole, slices + ["X+", "X-", "XF+", "XF-"], 6))
    for ab, first in enumerate("yz"):
        def finished(dz, dy, half, ab=ab):
            ref = ga.at[ab, row_block(ab, dz, dy)]
            return ref if half is None else ref.at[:, pl.ds(half * 512, 512)]

        have = spread("g%d" % ab, finished, 16 * 1024 * 2, first, ["XS"], GRAD_RANK)
        whole = sorted({n for dz in range(4) for dy in range(4) for n in have(dz, dy)})
        add("PH%d" % ab, "pair", 256 * 1024 * 2, ga.at[ab], gb.at[ab], gb.at[ab], whole)

    for item, rank in zip(copies + tasks, COPY_RANKS + TASK_RANKS, strict=True):
        item.rank = rank
    for item, rank in zip(copies + tasks, COPY_RANKS + TASK_RANKS, strict=True):
        item.rank = rank
    order, _ = arrange(copies, tasks, ["L", "LG", "LC"])
    assert len(copies) == COPIES
    place = {copy.name: i for i, copy in enumerate(copies)}
    by_name = {copy.name: copy for copy in copies}

    def descriptor(copy, landing):
        i = place[copy.name]
        return pltpu.make_async_remote_copy(
            src_ref=copy.source, dst_ref=landing, send_sem=send_sem.at[i], recv_sem=recv_sem.at[i],
            device_id=targets[copy.link], device_id_type=MESH)

    loads = [
        pltpu.make_async_copy(tokens, tok.at[0, 0], load_sem.at[0]),
        pltpu.make_async_copy(up.at[:, pl.ds(pl.multiple_of(xh * 896, 128), 896)], ub.at[plane(0, 0), xh], load_sem.at[1]),
        pltpu.make_async_copy(down.at[pl.ds(pl.multiple_of(xh * 896, 128), 896), :], db.at[plane(0, 0), xh], load_sem.at[2]),
    ]
    load_gate = pltpu.make_async_copy(gate.at[:, pl.ds(pl.multiple_of(xh * 896, 128), 896)], gw, load_sem.at[3])
    extra = [
        pltpu.make_async_copy(cotangent, cot, load_sem.at[4]),
        pltpu.make_async_copy(factors_down, fdown, load_sem.at[5]),
        pltpu.make_async_copy(factors_up, fup, load_sem.at[6]),
    ]
    for load in loads:
        load.start()
    for load in extra:
        load.start()
    load_gate.start()
    barrier = pltpu.get_barrier_semaphore()
    for target in targets.values():
        pl.semaphore_signal(barrier, inc=1, device_id=target, device_id_type=MESH)
    pl.semaphore_wait(barrier, len(targets))
    gate_waited = loads_waited = False
    used = []
    for what, item in order:
        if not loads_waited and "L" in item.after:
            for load in loads:
                load.wait()
            loads_waited = True
        if item.name[0] == "D" and what == "task":
            if len(used) >= SLOTS:
                early = by_name["Q" + used[-SLOTS]]
                descriptor(early, early.landing).wait_send()
            slot[int(item.name[1:])] = len(used) % SLOTS
            used.append(item.name[1:])
            by_name["Q" + used[-1]].source = psib.at[slot[int(used[-1])]]
        if what == "send":
            descriptor(item, item.landing).start()
        elif what == "recv":
            descriptor(item, item.here).wait_recv()
        else:
            if item.name[0] == "G" and not gate_waited:
                load_gate.wait()
                gate_waited = True
            if item.name == "W0":
                for load in extra:
                    load.wait()
            item.run()
    stores = []
    for half, whole in ((core, ga), (1 - core, gb)):
        for ab in range(2):
            columns = pl.ds(pl.multiple_of(half * 2048 + ab * 1024, 1024), 1024)
            for n, result in enumerate((grads_low, grads_high)):
                part = whole.at[ab, pl.ds(8 * n, 8)]
                stores.append(pltpu.make_async_copy(part, result.at[:, :, columns], load_sem.at[len(stores)]))
    for store in stores:
        store.start()
    already = {"Q" + n for n in used[:-SLOTS]} | {"PG00", "PG01"}
    for copy in copies:
        if copy.name not in already:
            descriptor(copy, copy.landing).wait_send()
    for store in stores:
        store.wait()


COPIES = 8 + 28 + 64 + 64 + 4 + 16 + 4 + 32 + 2


def layer(*operands):
    hbm = pl.BlockSpec(memory_space=pl.ANY)
    return pl.pallas_call(
        kernel,
        out_shape=(jax.ShapeDtypeStruct((128, 4096), BF), jax.ShapeDtypeStruct((8, 16, 4096), BF), jax.ShapeDtypeStruct((8, 16, 4096), BF)),
        in_specs=[hbm] * 7 + [pl.BlockSpec(memory_space=pltpu.VMEM)] * 3,
        out_specs=(pl.BlockSpec(memory_space=pltpu.VMEM), hbm, hbm),
        scratch_shapes=[
            pltpu.VMEM((4, 2, 128, 4096), BF),
            pltpu.VMEM((4096, 896), BF),
            pltpu.VMEM((16, 2, 128, 896), BF),
            pltpu.VMEM((16, 2, 896, 128), BF),
            pltpu.VMEM((4, 256, 896), F32),
            pltpu.VMEM((4, 256, 896), F32),
            pltpu.VMEM((4, 256, 896), BF),
            pltpu.VMEM((SLOTS, 4, 128, 256), BF),
            pltpu.VMEM((16, 4, 128, 256), BF),
            pltpu.VMEM((16, 4, 128, 256), BF),
            pltpu.VMEM((8, 128, 256), BF),
            pltpu.VMEM((8, 128, 256), BF),
            pltpu.VMEM((16, 128, 256), BF),
            pltpu.VMEM((16, 128, 256), BF),
            pltpu.VMEM((2, 64, 896), BF),
            pltpu.VMEM((2, 448, 128), BF),
            pltpu.VMEM((2, 256, 1152), F32),
            pltpu.VMEM((2, 128, 1152), F32),
            pltpu.VMEM((128, 4096), BF),
            pltpu.VMEM((4096, 128), BF),
            pltpu.VMEM((128, 4096), BF),
            pltpu.VMEM((128, 128), F32),
            pltpu.VMEM((128, 128), BF),
            pltpu.VMEM((2, 128, 128), BF),
            pltpu.VMEM((2, 2, 40, 1152), F32),
            pltpu.VMEM((2, 2, 80, 1152), F32),
            pltpu.VMEM((4, 2, 16, 1152), F32),
            pltpu.VMEM((2, 16, 16, 1024), BF),
            pltpu.VMEM((2, 16, 16, 1024), BF),
            pltpu.SemaphoreType.DMA((8,)),
            pltpu.SemaphoreType.DMA((COPIES,)),
            pltpu.SemaphoreType.DMA((COPIES,)),
        ],
        compiler_params=pltpu.CompilerParams(
            collective_id=0, has_side_effects=True, vmem_limit_bytes=67_000_000),
        cost_estimate=pl.CostEstimate(flops=22_500_000_000, bytes_accessed=16_000_000, transcendentals=1_000_000),
        name="layer",
    )(*operands)


def shards(
    tokens,
    gate_projection_weight,
    up_projection_weight,
    down_projection_weight,
    router_projection_weight,
    adapter_down_factors,
    adapter_up_factors,
    routes,
    padding_token_mask,
    cotangent,
):
    layer_out, grads_low, grads_high = layer(
        tokens, gate_projection_weight, up_projection_weight, down_projection_weight,
        cotangent, adapter_down_factors, adapter_up_factors, router_projection_weight.T, routes.T,
        padding_token_mask[None, :])
    unit = jnp.eye(128, dtype=BF)
    grad_down = lax.dot_general(grads_low.reshape(128, 4096), unit, (((0,), (0,)), ((), ())), preferred_element_type=F32)
    grad_up = grads_high.reshape(128, 4096).astype(F32)
    return (layer_out, grad_down, grad_up)


def solution(mesh):
    return jax.shard_map(
        shards,
        mesh=mesh,
        in_specs=(
            P(("dp", "blk"), None),
            P(None, "blk"),
            P("dp", "blk"),
            P("blk", "dp"),
            P(),
            P(),
            P(),
            P(("dp", "blk"), None),
            P(("dp", "blk")),
            P(("dp", "blk"), None),
        ),
        out_specs=(P(("dp", "blk"), None), P(), P()),
        check_vma=False,
    )
```
